8 devices in a mesh: dp: 1 (over z), ep: 8 (over y, x, core).
Axes of the slice: x: 2, y: 2, z: 1, core: 2. Of those that a mesh axis runs over, the one named last changes fastest.
Arguments:
- hidden: bfloat16 [2048, 1024], P(('dp', 'ep'))
- k_cache: bfloat16 [2048, 128, 8, 64], P(('dp', 'ep'))
- v_cache: bfloat16 [2048, 128, 8, 64], P(('dp', 'ep'))
- seq_lens: int32 [2048], P(('dp', 'ep'))
- expert_ids: int32 [2048, 8], P(('dp', 'ep'))
- ln_attn: bfloat16 [1024], replicated
- w_q: bfloat16 [1024, 1024], replicated
- w_k: bfloat16 [1024, 512], replicated
- w_v: bfloat16 [1024, 512], replicated
- q_gain: bfloat16 [64], replicated
- k_gain: bfloat16 [64], replicated
- w_o: bfloat16 [1024, 1024], replicated
- ln_moe: bfloat16 [1024], replicated
- w_router: bfloat16 [1024, 32], replicated
- w_gate: bfloat16 [32, 1024, 512], P('ep')
- w_up: bfloat16 [32, 1024, 512], P('ep')
- w_down: bfloat16 [32, 512, 1024], P('ep')
Outputs:
- output 1: bfloat16 [2048, 1024], P(('dp', 'ep'))
- output 2: bfloat16 [2048, 128, 8, 64], P(('dp', 'ep'))
- output 3: bfloat16 [2048, 128, 8, 64], P(('dp', 'ep'))
All inputs are finite; a program needn't handle non-finite values.
Results may differ from the reference program's by a relative error of at most 0.0112857.
Values are sent between devices in bfloat16 or wider.
A program may use at most 1 GiB of HBM per device.

```python
import jax
import jax.numpy as jnp
import numpy as np
from jax import lax

D = 1024
HEADS = 16
KV_HEADS = 8
HEAD = 64
EXPERTS = 32
FF = 512
TOP = 8
ROPE_BASE = 1000000
TMAX = 128
SEQ_DEV = 256
GROUP = 8

BATCH = SEQ_DEV * GROUP
CAP = 2 * SEQ_DEV // (EXPERTS // TOP)
EPS = 1e-6


def draw_routing(route_key):
    group_width = EXPERTS // TOP
    pos_table = np.array([0 if tok_num < CAP else 1 + (tok_num - CAP) % (group_width - 1) for tok_num in range(SEQ_DEV)], dtype=np.int32)
    perm_key, tok_key = jax.random.split(route_key)
    expert_perm = jax.random.permutation(perm_key, EXPERTS).astype(jnp.int32)
    tok_keys = jax.random.split(tok_key, GROUP * TOP)
    tok_perms = jax.vmap(lambda one_key: jax.random.permutation(one_key, SEQ_DEV))(tok_keys)
    positions = jnp.asarray(pos_table)[tok_perms].reshape(GROUP, TOP, SEQ_DEV)
    offsets = (jnp.arange(TOP, dtype=jnp.int32) * group_width)[None, :, None]
    chosen_ids = expert_perm[offsets + positions]
    return jnp.transpose(chosen_ids, (0, 2, 1)).reshape(BATCH, TOP).astype(jnp.int32)


def draw_lens(len_key):
    spread_key, raw_key = jax.random.split(len_key)
    spread = jax.random.randint(spread_key, (GROUP, 1), 1, 5)
    raw_lens = jax.random.randint(raw_key, (GROUP, SEQ_DEV), 0, TMAX)
    seq_lens = (raw_lens * spread // 4).reshape(BATCH)
    return seq_lens.at[0].set(TMAX - 1).astype(jnp.int32)


def setup_inputs(seed: int = 0, part: int = 0) -> dict:
    base_key = jax.random.key(seed)
    shared_keys = jax.random.split(base_key, 12)
    part_keys = jax.random.split(jax.random.fold_in(base_key, part), 5)
    hidden = jax.random.normal(part_keys[0], (BATCH, D), jnp.float32).astype(jnp.bfloat16)
    k_cache = (1.5 * jax.random.normal(part_keys[1], (BATCH, TMAX, KV_HEADS, HEAD), jnp.float32)).astype(jnp.bfloat16)
    v_cache = jax.random.normal(part_keys[2], (BATCH, TMAX, KV_HEADS, HEAD), jnp.float32).astype(jnp.bfloat16)
    seq_lens = draw_lens(part_keys[3])
    expert_ids = draw_routing(part_keys[4])
    ln_attn = (1.0 + 0.2 * jax.random.normal(shared_keys[0], (D,), jnp.float32)).astype(jnp.bfloat16)
    w_q = (jax.random.normal(shared_keys[1], (D, HEADS * HEAD), jnp.float32) * D ** -0.5).astype(jnp.bfloat16)
    w_k = (jax.random.normal(shared_keys[2], (D, KV_HEADS * HEAD), jnp.float32) * D ** -0.5).astype(jnp.bfloat16)
    w_v = (jax.random.normal(shared_keys[3], (D, KV_HEADS * HEAD), jnp.float32) * D ** -0.5).astype(jnp.bfloat16)
    q_gain = (1.6 + 0.3 * jax.random.normal(shared_keys[4], (HEAD,), jnp.float32)).astype(jnp.bfloat16)
    k_gain = (1.6 + 0.3 * jax.random.normal(shared_keys[5], (HEAD,), jnp.float32)).astype(jnp.bfloat16)
    w_o = (jax.random.normal(shared_keys[6], (HEADS * HEAD, D), jnp.float32) * (HEADS * HEAD) ** -0.5).astype(jnp.bfloat16)
    ln_moe = (1.0 + 0.2 * jax.random.normal(shared_keys[7], (D,), jnp.float32)).astype(jnp.bfloat16)
    w_router = (2.0 * jax.random.normal(shared_keys[8], (D, EXPERTS), jnp.float32) * D ** -0.5).astype(jnp.bfloat16)
    w_gate = (jax.random.normal(shared_keys[9], (EXPERTS, D, FF), jnp.float32) * D ** -0.5).astype(jnp.bfloat16)
    w_up = (jax.random.normal(shared_keys[10], (EXPERTS, D, FF), jnp.float32) * D ** -0.5).astype(jnp.bfloat16)
    w_down = (2.0 * jax.random.normal(shared_keys[11], (EXPERTS, FF, D), jnp.float32) * FF ** -0.5).astype(jnp.bfloat16)
    return {'hidden': hidden, 'k_cache': k_cache, 'v_cache': v_cache, 'seq_lens': seq_lens, 'expert_ids': expert_ids, 'ln_attn': ln_attn, 'w_q': w_q, 'w_k': w_k, 'w_v': w_v, 'q_gain': q_gain, 'k_gain': k_gain, 'w_o': w_o, 'ln_moe': ln_moe, 'w_router': w_router, 'w_gate': w_gate, 'w_up': w_up, 'w_down': w_down}


def rms_scale(values, gain_vec):
    mean_sq = jnp.mean(values * values, axis=-1, keepdims=True)
    return values * lax.rsqrt(mean_sq + EPS) * gain_vec.astype(jnp.float32)


def rotate_half(values, angles):
    half_dim = values.shape[-1] // 2
    x_low = values[..., :half_dim]
    x_high = values[..., half_dim:]
    cos_val = jnp.cos(angles)
    sin_val = jnp.sin(angles)
    return jnp.concatenate([x_low * cos_val - x_high * sin_val, x_high * cos_val + x_low * sin_val], axis=-1)


def attend(hidden, k_cache, v_cache, seq_lens, ln_attn, w_q, w_k, w_v, q_gain, k_gain, w_o):
    n_seq = hidden.shape[0]
    h_f32 = hidden.astype(jnp.float32)
    x_norm = rms_scale(h_f32, ln_attn).astype(jnp.bfloat16)
    q_proj = jnp.dot(x_norm, w_q, preferred_element_type=jnp.float32).reshape(n_seq, HEADS, HEAD)
    k_proj = jnp.dot(x_norm, w_k, preferred_element_type=jnp.float32).reshape(n_seq, KV_HEADS, HEAD)
    v_new = jnp.dot(x_norm, w_v, preferred_element_type=jnp.float32).astype(jnp.bfloat16).reshape(n_seq, KV_HEADS, HEAD)
    inv_freq = jnp.power(float(ROPE_BASE), -jnp.arange(0, HEAD, 2).astype(jnp.float32) / HEAD)
    angles = seq_lens.astype(jnp.float32)[:, None, None] * inv_freq[None, None, :]
    q_rot = rotate_half(rms_scale(q_proj, q_gain), angles).astype(jnp.bfloat16)
    k_new = rotate_half(rms_scale(k_proj, k_gain), angles).astype(jnp.bfloat16)
    positions = jnp.arange(TMAX, dtype=jnp.int32)
    at_slot = (positions[None, :] == seq_lens[:, None])[:, :, None, None]
    k_all = jnp.where(at_slot, k_new[:, None], k_cache)
    v_all = jnp.where(at_slot, v_new[:, None], v_cache)
    q_grp = q_rot.reshape(n_seq, KV_HEADS, HEADS // KV_HEADS, HEAD)
    scores = jnp.einsum('skgd,stkd->skgt', q_grp.astype(jnp.float32), k_all.astype(jnp.float32)) * (HEAD ** -0.5)
    visible = (positions[None, :] <= seq_lens[:, None])[:, None, None, :]
    scores = jnp.where(visible, scores, -1e30)
    att_probs = jax.nn.softmax(scores, axis=-1).astype(jnp.bfloat16)
    attn_out = jnp.einsum('skgt,stkd->skgd', att_probs.astype(jnp.float32), v_all.astype(jnp.float32))
    attn_out = attn_out.astype(jnp.bfloat16).reshape(n_seq, HEADS * HEAD)
    y_res = h_f32 + jnp.dot(attn_out, w_o, preferred_element_type=jnp.float32)
    return y_res, k_all, v_all


def reference(hidden, k_cache, v_cache, seq_lens, expert_ids, ln_attn, w_q, w_k, w_v, q_gain, k_gain, w_o, ln_moe, w_router, w_gate, w_up, w_down):
    def block_attn(block_in):
        h_blk, kc_blk, vc_blk, len_blk = block_in
        return attend(h_blk, kc_blk, vc_blk, len_blk, ln_attn, w_q, w_k, w_v, q_gain, k_gain, w_o)

    y_blocks, k_blocks, v_blocks = lax.map(block_attn, (hidden.reshape(GROUP, SEQ_DEV, D), k_cache.reshape(GROUP, SEQ_DEV, TMAX, KV_HEADS, HEAD), v_cache.reshape(GROUP, SEQ_DEV, TMAX, KV_HEADS, HEAD), seq_lens.reshape(GROUP, SEQ_DEV)))
    y_res = y_blocks.reshape(BATCH, D)
    k_all = k_blocks.reshape(BATCH, TMAX, KV_HEADS, HEAD)
    v_all = v_blocks.reshape(BATCH, TMAX, KV_HEADS, HEAD)

    r_norm = rms_scale(y_res, ln_moe).astype(jnp.bfloat16)
    logits = jnp.dot(r_norm, w_router, preferred_element_type=jnp.float32)
    gate_vals = jax.nn.softmax(jnp.take_along_axis(logits, expert_ids, axis=1), axis=-1)

    n_pairs = BATCH * TOP
    per_expert = GROUP * CAP
    flat_ids = expert_ids.reshape(n_pairs)
    sort_order = jnp.argsort(flat_ids, stable=True)
    sorted_tok = (sort_order // TOP).astype(jnp.int32)
    counts = jnp.bincount(flat_ids, length=EXPERTS).astype(jnp.int32)
    starts = jnp.cumsum(counts) - counts
    tok_padded = jnp.concatenate([sorted_tok, jnp.zeros((per_expert,), jnp.int32)])

    def run_expert(expert_in):
        start_at, w_gate_e, w_up_e, w_down_e = expert_in
        tok_idx = lax.dynamic_slice(tok_padded, (start_at,), (per_expert,))
        tok_rows = jnp.take(r_norm, tok_idx, axis=0)
        gate_pre = jnp.dot(tok_rows, w_gate_e, preferred_element_type=jnp.float32)
        up_pre = jnp.dot(tok_rows, w_up_e, preferred_element_type=jnp.float32)
        hidden_act = (jax.nn.silu(gate_pre) * up_pre).astype(jnp.bfloat16)
        return jnp.dot(hidden_act, w_down_e, preferred_element_type=jnp.float32).astype(jnp.bfloat16)

    expert_out = lax.map(run_expert, (starts, w_gate, w_up, w_down))
    inverse = jnp.argsort(sort_order)
    pair_rank = inverse - starts[flat_ids]
    picked = expert_out[flat_ids, pair_rank].reshape(BATCH, TOP, D).astype(jnp.float32)
    moe_out = jnp.sum(gate_vals[:, :, None] * picked, axis=1)
    return (y_res + moe_out).astype(jnp.bfloat16), k_all, v_all
```

```python
import functools
import numpy as np
import jax, jax.numpy as jnp
from jax import lax
from jax.experimental import pallas as pl
from jax.experimental.pallas import tpu as pltpu
from jax.sharding import PartitionSpec as P
EPS=1e-6; ROPE_BASE=1e6
F32=jnp.float32; BF=jnp.bfloat16

def attn_body(cfg, lens_s, lens_ref, ids_ref, vec_ref, gain_ref, freq_ref, h_hbm, wq_hbm, wk_hbm, wv_hbm, wo_hbm, wr_ref, k_hbm, v_hbm,
              ko_hbm, vo_hbm, y_ref, r_ref, gt_ref,
              kb, vb, wq, wk, wv, woe, woo, h_ref, qe_ref, qo_ref, kt_ref, vt_ref, ae_ref, ao_ref, isem, osem, wsem):
    sb, nb, lag = cfg
    n = h_ref.shape[0]
    steps = n // sb
    per = 128 // sb
    n_kv, hd, dk = 8, 64, 512
    def cin(g, which):
        s = lax.rem(g, nb)
        r, b = ((k_hbm, kb), (v_hbm, vb))[which]
        return pltpu.make_async_copy(r.at[pl.ds(g*sb, sb)], b.at[s], isem.at[which, s])
    def cout(g, which):
        s = lax.rem(g, nb)
        r, b = ((ko_hbm, kb), (vo_hbm, vb))[which]
        return pltpu.make_async_copy(b.at[s], r.at[pl.ds(g*sb, sb)], osem.at[which, s])
    wcopies = [pltpu.make_async_copy(a, b, wsem.at[i]) for i, (a, b) in enumerate(
        ((h_hbm, h_ref), (wq_hbm, wq), (wk_hbm, wk), (wv_hbm, wv), (wo_hbm.at[:, 0], woe), (wo_hbm.at[:, 1], woo)))]
    for c in wcopies[:4]:
        c.start()
    for g in range(nb):
        cin(g, 0).start(); cin(g, 1).start()
    for c in wcopies[4:]:
        c.start()
    for c in wcopies[:4]:
        c.wait()
    h = h_ref[...].astype(F32)
    x = (h * lax.rsqrt(jnp.mean(h*h, axis=-1, keepdims=True) + EPS) * vec_ref[0:1, :]).astype(BF)
    ang = freq_ref[...] * lens_ref[...].astype(F32)
    cos_v = jnp.cos(ang)[None]; sin_v = jnp.sin(ang)[None]
    half = hd // 2
    def norm_rope(w_ref, gain):
        p = jnp.dot(x, w_ref[...], preferred_element_type=F32)
        p = p.T.reshape(-1, hd, n)
        p = p * lax.rsqrt(jnp.mean(p*p, axis=1, keepdims=True) + EPS) * gain[None]
        lo, hi = p[:, :half], p[:, half:]
        return jnp.concatenate([lo*cos_v - hi*sin_v, hi*cos_v + lo*sin_v], axis=1)
    q = norm_rope(wq, gain_ref[:, 0:1])
    q = q.reshape(n_kv, 2, hd, n)
    qe_ref[...] = q[:, 0].reshape(dk, n).T
    qo_ref[...] = q[:, 1].reshape(dk, n).T
    k = norm_rope(wk, gain_ref[:, 1:2]).reshape(dk, n).astype(BF).astype(F32)
    v = jnp.dot(x, wv[...], preferred_element_type=F32).T.astype(BF).astype(F32)
    for c in range(n // 128):
        kt_ref[c] = k[:, 128*c:128*c+128]
        vt_ref[c] = v[:, 128*c:128*c+128]

    lane = lax.broadcasted_iota(jnp.int32, (1, 128), 1)
    row = lax.broadcasted_iota(jnp.int32, (16, dk), 0)
    col = lax.broadcasted_iota(jnp.int32, (16, dk), 1) // hd
    m_even = row == col
    m_odd = row == col + n_kv

    @pl.loop(0, steps)
    def _(g):
        slot = lax.rem(g, nb)
        @pl.when((g >= lag) & (g - lag + nb < steps))
        def _():
            cout(g - lag, 0).wait(); cout(g - lag, 1).wait()
            cin(g - lag + nb, 0).start(); cin(g - lag + nb, 1).start()
        cin(g, 0).wait(); cin(g, 1).wait()
        base = lax.rem(g, per) * sb
        hf = g // per
        rows = pl.ds(pl.multiple_of(g*sb, sb), sb)
        qe = qe_ref[rows, :]
        qo = qo_ref[rows, :]
        hits = []; sc = []
        for p in range(sb // 2):
            ks = []; qs = []
            for i in (2*p, 2*p+1):
                ln = lens_s[g*sb + i]
                hits.append(lane == ln)
                kc = pltpu.roll(kt_ref[hf], lax.rem(ln - (base + i) + 128, 128), 1).astype(BF)
                kn = jnp.where(hits[i], kc, kb[slot, i])
                kb[slot, i] = kn
                ks.append(kn)
                qs.append(jnp.where(m_even, qe[i:i+1], jnp.where(m_odd, qo[i:i+1], 0.0)).astype(BF))
            s = jnp.dot(jnp.concatenate(qs, axis=0), jnp.concatenate(ks, axis=1), preferred_element_type=F32)
            for j in (0, 1):
                vis = lane <= lens_s[g*sb + 2*p + j]
                sc.append(jnp.where(vis, s[16*j:16*j+16, 128*j:128*j+128] * (hd ** -0.5), -1e30))
        cout(g, 0).start()
        for i in range(sb):
            ln = lens_s[g*sb + i]
            vc = pltpu.roll(vt_ref[hf], lax.rem(ln - (base + i) + 128, 128), 1).astype(BF)
            vb[slot, i] = jnp.where(hits[i], vc, vb[slot, i])
        cout(g, 1).start()
        s = jnp.concatenate(sc, axis=0)
        e = jnp.exp(s - jnp.max(s, axis=-1, keepdims=True))
        pr = (e / jnp.sum(e, axis=-1, keepdims=True)).astype(BF)
        zz = jnp.zeros((16, 128), BF)
        oe = []; oo = []
        for p in range(sb // 2):
            p0 = pr[32*p:32*p+16]; p1 = pr[32*p+16:32*p+32]
            pp = jnp.concatenate([jnp.concatenate([p0, zz], axis=1), jnp.concatenate([zz, p1], axis=1)], axis=0)
            vv = jnp.concatenate([vb[slot, 2*p], vb[slot, 2*p+1]], axis=1)
            o = lax.dot_general(pp, vv, (((1,), (1,)), ((), ())), preferred_element_type=F32)
            for j in (0, 1):
                oj = o[16*j:16*j+16]
                oe.append(jnp.sum(jnp.where(m_even[:8], oj[:8], 0.0), axis=0, keepdims=True))
                oo.append(jnp.sum(jnp.where(m_even[:8], oj[8:], 0.0), axis=0, keepdims=True))
        ae_ref[rows, :] = jnp.concatenate(oe, axis=0)
        ao_ref[rows, :] = jnp.concatenate(oo, axis=0)

    for c in wcopies[4:]:
        c.wait()
    y = h_ref[...].astype(F32)
    y = y + (jnp.dot(ae_ref[...].astype(BF), woe[...].reshape(dk, -1), preferred_element_type=F32)
             + jnp.dot(ao_ref[...].astype(BF), woo[...].reshape(dk, -1), preferred_element_type=F32))
    y_ref[...] = y
    r = (y * lax.rsqrt(jnp.mean(y*y, axis=-1, keepdims=True) + EPS) * vec_ref[1:2, :]).astype(BF)
    r_ref[...] = r
    lg = lax.dot_general(wr_ref[...], r, (((1,), (1,)), ((), ())), preferred_element_type=F32)
    eid = lax.broadcasted_iota(jnp.int32, lg.shape, 0)
    ids = ids_ref[...]
    hot = eid == ids[0:1]
    for j in range(1, ids.shape[0]):
        hot = hot | (eid == ids[j:j+1])
    lg = jnp.where(hot, lg, -jnp.inf)
    e = jnp.where(hot, jnp.exp(lg - jnp.max(lg, axis=0, keepdims=True)), 0.0)
    gt_ref[...] = e / jnp.sum(e, axis=0, keepdims=True)
    for j in range(nb):
        cout(steps - nb + j, 0).wait(); cout(steps - nb + j, 1).wait()

def attn_call(hidden, k_cache, v_cache, seq_lens, expert_ids, ln_attn, w_q, w_k, w_v, q_gain, k_gain, w_o, ln_moe, w_router, cfg=(8, 8, 3)):
    n, d = hidden.shape
    t = k_cache.shape[1]; dk = w_k.shape[1]; hd = q_gain.shape[0]; nk = dk // hd
    kc = k_cache.transpose(0, 2, 3, 1).reshape(n, dk, t)
    vc = v_cache.transpose(0, 2, 3, 1).reshape(n, dk, t)
    vec = jnp.stack([ln_attn, ln_moe]).astype(F32)
    gain = jnp.stack([q_gain, k_gain], axis=1).astype(F32)
    freq = jnp.asarray(np.power(np.float32(ROPE_BASE), -np.arange(0, hd, 2).astype(np.float32) / np.float32(hd)).astype(np.float32).reshape(-1, 1))
    sb, nb, lag = cfg
    vm = pl.BlockSpec(memory_space=pltpu.VMEM)
    an = pl.BlockSpec(memory_space=pl.ANY)
    sm = pl.BlockSpec(memory_space=pltpu.SMEM)
    ne = w_router.shape[1]
    out = pl.pallas_call(functools.partial(attn_body, cfg),
        out_shape=(jax.ShapeDtypeStruct(kc.shape, BF), jax.ShapeDtypeStruct(vc.shape, BF), jax.ShapeDtypeStruct((n, d), F32),
                   jax.ShapeDtypeStruct((n, d), BF), jax.ShapeDtypeStruct((ne, n), F32)),
        in_specs=[sm, vm, vm, vm, vm, vm, an, an, an, an, an, vm, an, an],
        out_specs=(an, an, vm, vm, vm),
        scratch_shapes=[pltpu.VMEM((nb, sb, dk, t), BF), pltpu.VMEM((nb, sb, dk, t), BF),
            pltpu.VMEM(w_q.shape, BF), pltpu.VMEM(w_k.shape, BF), pltpu.VMEM(w_v.shape, BF),
            pltpu.VMEM((nk, hd, d), BF), pltpu.VMEM((nk, hd, d), BF), pltpu.VMEM((n, d), BF),
            pltpu.VMEM((n, dk), F32), pltpu.VMEM((n, dk), F32), pltpu.VMEM((n//128, dk, 128), F32), pltpu.VMEM((n//128, dk, 128), F32),
            pltpu.VMEM((n, dk), F32), pltpu.VMEM((n, dk), F32),
            pltpu.SemaphoreType.DMA((2, nb)), pltpu.SemaphoreType.DMA((2, nb)), pltpu.SemaphoreType.DMA((6,))],
        compiler_params=pltpu.CompilerParams(vmem_limit_bytes=60<<20), name="attn",
        cost_estimate=pl.CostEstimate(flops=8*10**9, bytes_accessed=140*10**6, transcendentals=0),
    )(seq_lens, seq_lens.reshape(1, n), expert_ids.T, vec, gain, freq, hidden, w_q, w_k, w_v,
      w_o.reshape(nk, 2, hd, d), w_router.T, kc, vc)
    ko, vo, y, r, gt = out
    back = lambda z: z.reshape(n, nk, hd, t).transpose(0, 3, 1, 2)
    return back(ko), back(vo), y, r, gt


def moe_body(r_ref, gt_ref, y_ref, wg_own, wu_own, wd_own, wg_par, wu_par, wd_par, out_ref,
             wg, wu, wd, xr, gts, acc, rbuf, wsem, agsem_s, agsem_r, rssem_s, rssem_r):
    me = lax.axis_index('ep')
    core = me % 2
    xpos = (me // 2) % 2
    ypos = me // 4
    peers = [None, ypos*4 + (1-xpos)*2 + core, (1-ypos)*4 + xpos*2 + core, (1-ypos)*4 + (1-xpos)*2 + core]
    n_loc = wg_own.shape[0]
    n_exp = 2*n_loc
    half = acc.shape[-1]
    n = acc.shape[2]

    def wcopy(e, own):
        src = (wg_own, wu_own, wd_own) if own else (wg_par, wu_par, wd_par)
        s = lax.rem(e, n_loc)
        return [pltpu.make_async_copy(a.at[s], b.at[e], wsem.at[i, e]) for i, (a, b) in enumerate(zip(src, (wg, wu, wd)))]
    for e in range(n_exp):
        for c in wcopy(jnp.int32(e), e < n_loc):
            c.start()

    barrier = pltpu.get_barrier_semaphore()
    for p in peers[1:]:
        pl.semaphore_signal(barrier, inc=1, device_id={"ep": p}, device_id_type=pl.DeviceIdType.MESH)
    pl.semaphore_wait(barrier, 3)

    def remote(src, dst, ss, rs, p):
        return pltpu.make_async_remote_copy(src_ref=src, dst_ref=dst, send_sem=ss, recv_sem=rs,
                                            device_id={"ep": p}, device_id_type=pl.DeviceIdType.MESH)
    ag = {}
    for b in (3, 1, 2):
        rows8 = pl.ds(pl.multiple_of((peers[b] // 2) * n_exp, n_exp), n_exp)
        ag[b] = [remote(r_ref, xr.at[b-1], agsem_s.at[0, b-1], agsem_r.at[0, b-1], peers[b]),
                 remote(gt_ref.at[rows8], gts.at[b-1], agsem_s.at[1, b-1], agsem_r.at[1, b-1], peers[b])]
        for c in ag[b]:
            c.start()

    lane8 = lax.broadcasted_iota(jnp.int32, (n, n_exp), 1)

    def compute(b, first):
        x_view = r_ref if b == 0 else xr.at[b-1]
        if b == 0:
            g8 = gt_ref[pl.ds(pl.multiple_of((me // 2) * n_exp, n_exp), n_exp), :]
        else:
            g8 = gts[b-1]
        g8 = g8.T
        def step(e, carry):
            if first:
                for c in wcopy(e, True):
                    c.wait()
            grow = lax.rem(core * n_loc + e, n_exp)
            gcol = jnp.sum(jnp.where(lane8 == grow, g8, 0.0), axis=1, keepdims=True)
            x = x_view[...]
            g = jnp.dot(x, wg[e], preferred_element_type=F32)
            u = jnp.dot(x, wu[e], preferred_element_type=F32)
            act = (jax.nn.silu(g) * u).astype(BF)
            for hf in (0, 1):
                f = jnp.dot(act, wd[e, :, hf*half:(hf+1)*half], preferred_element_type=F32).astype(BF).astype(F32)
                acc[b, hf] = acc[b, hf] + gcol * f
            return carry
        acc[b] = jnp.zeros(acc.shape[1:], F32)
        lax.fori_loop(0, n_exp, step, 0)

    def rs(i, src, p):
        return remote(src, rbuf.at[i], rssem_s.at[i], rssem_r.at[i], p)
    for c in ag[3]:
        c.wait_recv()
    compute(3, True)
    c_xd = rs(0, acc.at[3, 0], peers[1]); c_xd.start()
    c_yd = rs(1, acc.at[3, 1], peers[2]); c_yd.start()
    for c in ag[1]:
        c.wait_recv()
    compute(1, False)
    c_xa = rs(2, acc.at[1, 0], peers[1]); c_xa.start()
    for c in ag[2]:
        c.wait_recv()
    compute(2, False)
    c_yb = rs(3, acc.at[2, 1], peers[2]); c_yb.start()
    c_yd.wait_recv()
    acc[1, 1] = acc[1, 1] + rbuf[1]
    c_xb = rs(4, acc.at[1, 1], peers[1]); c_xb.start()
    c_xd.wait_recv()
    acc[2, 0] = acc[2, 0] + rbuf[0]
    c_ya = rs(5, acc.at[2, 0], peers[2]); c_ya.start()
    compute(0, False)
    c_xa.wait_recv()
    c_ya.wait_recv()
    out_ref[:, :half] = (y_ref[:, :half] + ((acc[0, 0] + rbuf[2]) + rbuf[5])).astype(out_ref.dtype)
    c_yb.wait_recv()
    c_xb.wait_recv()
    out_ref[:, half:] = (y_ref[:, half:] + ((acc[0, 1] + rbuf[3]) + rbuf[4])).astype(out_ref.dtype)
    for b in (1, 2, 3):
        for c in ag[b]:
            c.wait_send()
    for c in (c_xd, c_yd, c_xa, c_yb, c_xb, c_ya):
        c.wait_send()

def moe_call(r, gt, y, w_gate, w_up, w_down, wg_p, wu_p, wd_p):
    n, d = r.shape
    nl, _, ff = w_gate.shape
    vm = pl.BlockSpec(memory_space=pltpu.VMEM)
    an = pl.BlockSpec(memory_space=pl.ANY)
    dma = pltpu.SemaphoreType.DMA
    return pl.pallas_call(moe_body,
        out_shape=jax.ShapeDtypeStruct((n, d), BF),
        in_specs=[vm, vm, vm] + [an]*6, out_specs=vm,
        scratch_shapes=[pltpu.VMEM((2*nl, d, ff), BF), pltpu.VMEM((2*nl, d, ff), BF), pltpu.VMEM((2*nl, ff, d), BF),
            pltpu.VMEM((3, n, d), BF), pltpu.VMEM((3, 2*nl, n), F32), pltpu.VMEM((4, 2, n, d//2), F32), pltpu.VMEM((6, n, d//2), F32),
            dma((3, 2*nl)), dma((2, 3)), dma((2, 3)), dma((6,)), dma((6,))],
        compiler_params=pltpu.CompilerParams(vmem_limit_bytes=60<<20, collective_id=1, has_side_effects=True), name="moe",
        cost_estimate=pl.CostEstimate(flops=26*10**9, bytes_accessed=30*10**6, transcendentals=0),
    )(r, gt, y, w_gate, w_up, w_down, wg_p, wu_p, wd_p)


def solution(mesh):
    n_group = mesh.shape['ep']
    row_spec = P(('dp', 'ep'), None)
    cache_spec = P(('dp', 'ep'), None, None, None)
    len_spec = P(('dp', 'ep'))
    rep_vec = P(None)
    rep_mat = P(None, None)
    exp_spec = P('ep', None, None)
    swap = [(i, i + 1 - 2 * (i % 2)) for i in range(n_group)]

    def local_step(hidden, k_cache, v_cache, seq_lens, expert_ids, ln_attn, w_q, w_k, w_v, q_gain, k_gain, w_o, ln_moe, w_router, w_gate, w_up, w_down):
        wg_p = lax.ppermute(w_gate, 'ep', swap)
        wu_p = lax.ppermute(w_up, 'ep', swap)
        wd_p = lax.ppermute(w_down, 'ep', swap)
        k_all, v_all, y_res, r_norm, gates = attn_call(hidden, k_cache, v_cache, seq_lens, expert_ids, ln_attn, w_q, w_k, w_v, q_gain, k_gain, w_o, ln_moe, w_router)
        out = moe_call(r_norm, gates, y_res, w_gate, w_up, w_down, wg_p, wu_p, wd_p)
        return out, k_all, v_all

    return jax.shard_map(local_step, mesh=mesh, in_specs=(row_spec, cache_spec, cache_spec, len_spec, row_spec, rep_vec, rep_mat, rep_mat, rep_mat, rep_vec, rep_vec, rep_mat, rep_vec, rep_mat, exp_spec, exp_spec, exp_spec), out_specs=(row_spec, cache_spec, cache_spec), check_vma=False)
```

```python
import functools
import numpy as np
import jax, jax.numpy as jnp
from jax import lax
from jax.experimental import pallas as pl
from jax.experimental.pallas import tpu as pltpu
from jax.sharding import PartitionSpec as P
EPS=1e-6; ROPE_BASE=1e6
F32=jnp.float32; BF=jnp.bfloat16

def attn_body(cfg, lens_s, lens_ref, ids_ref, vec_ref, gain_ref, freq_ref, h_hbm, wq_hbm, wk_hbm, wv_hbm, wo_hbm, wr_ref, k_hbm, v_hbm, *refs):
    sb, nb, lag, lo, later = cfg
    gp_ref = None
    if later:
        gp_ref = refs[2]
        refs = refs[3:]
    (ko_hbm, vo_hbm, y_ref, r_ref, gt_ref,
     kb, vb, wq, wk, wv, woe, woo, h_ref, qe_ref, qo_ref, kt_ref, vt_ref, ae_ref, ao_ref, isem, osem, wsem) = refs
    n = h_ref.shape[0]
    steps = n // sb
    per = 128 // sb
    n_kv, hd, dk = 8, 64, 512
    def cin(g, which):
        s = lax.rem(g, nb)
        r, b = ((k_hbm, kb), (v_hbm, vb))[which]
        return pltpu.make_async_copy(r.at[pl.ds(lo + g*sb, sb)], b.at[s], isem.at[which, s])
    def cout(g, which):
        s = lax.rem(g, nb)
        r, b = ((ko_hbm, kb), (vo_hbm, vb))[which]
        return pltpu.make_async_copy(b.at[s], r.at[pl.ds(lo + g*sb, sb)], osem.at[which, s])
    wcopies = [pltpu.make_async_copy(a, b, wsem.at[i]) for i, (a, b) in enumerate(
        ((h_hbm.at[pl.ds(lo, n)], h_ref), (wq_hbm, wq), (wk_hbm, wk), (wv_hbm, wv), (wo_hbm.at[:, 0], woe), (wo_hbm.at[:, 1], woo)))]
    for c in wcopies[:4]:
        c.start()
    for c in wcopies[:4]:
        c.wait()
    for g in range(nb):
        cin(g, 0).start(); cin(g, 1).start()
    for c in wcopies[4:]:
        c.start()
    h = h_ref[...].astype(F32)
    x = (h * lax.rsqrt(jnp.mean(h*h, axis=-1, keepdims=True) + EPS) * vec_ref[0:1, :]).astype(BF)
    ang = freq_ref[...] * lens_ref[:, lo:lo+n].astype(F32)
    cos_v = jnp.cos(ang)[None]; sin_v = jnp.sin(ang)[None]
    half = hd // 2
    def norm_rope(w_ref, gain):
        p = jnp.dot(x, w_ref[...], preferred_element_type=F32)
        p = p.T.reshape(-1, hd, n)
        p = p * lax.rsqrt(jnp.mean(p*p, axis=1, keepdims=True) + EPS) * gain[None]
        lo, hi = p[:, :half], p[:, half:]
        return jnp.concatenate([lo*cos_v - hi*sin_v, hi*cos_v + lo*sin_v], axis=1)
    q = norm_rope(wq, gain_ref[:, 0:1])
    q = q.reshape(n_kv, 2, hd, n)
    qe_ref[...] = q[:, 0].reshape(dk, n).T
    qo_ref[...] = q[:, 1].reshape(dk, n).T
    k = norm_rope(wk, gain_ref[:, 1:2]).reshape(dk, n).astype(BF).astype(F32)
    v = jnp.dot(x, wv[...], preferred_element_type=F32).T.astype(BF).astype(F32)
    for c in range(0, n, 128):
        w = min(128, n - c)
        kt_ref[c // 128, :, :w] = k[:, c:c+w]
        vt_ref[c // 128, :, :w] = v[:, c:c+w]

    lane = lax.broadcasted_iota(jnp.int32, (1, 128), 1)
    row = lax.broadcasted_iota(jnp.int32, (16, dk), 0)
    col = lax.broadcasted_iota(jnp.int32, (16, dk), 1) // hd
    m_even = row == col
    m_odd = row == col + n_kv

    zz = jnp.zeros((16, 128), BF)
    def fresh(t_ref, g, i):
        ln = lens_s[lo + g*sb + i]
        col = pltpu.roll(t_ref[g // per], lax.rem(ln - (lax.rem(g, per) * sb + i) + 128, 128), 1).astype(BF)
        return lane == ln, col
    def insert(buf, t_ref, g, p):
        slot = lax.rem(g, nb)
        for i in (2*p, 2*p+1):
            hit, col = fresh(t_ref, g, i)
            buf[slot, i] = jnp.where(hit, col, buf[slot, i])
    def scores(g, p, qe, qo):
        slot = lax.rem(g, nb)
        qs = [jnp.where(m_even, qe[i:i+1], jnp.where(m_odd, qo[i:i+1], 0.0)).astype(BF) for i in (2*p, 2*p+1)]
        ks = jnp.concatenate([kb[slot, 2*p], kb[slot, 2*p+1]], axis=1)
        s = jnp.dot(jnp.concatenate(qs, axis=0), ks, preferred_element_type=F32)
        return [jnp.where(lane <= lens_s[lo + g*sb + 2*p + j], s[16*j:16*j+16, 128*j:128*j+128] * (hd ** -0.5), -1e30) for j in (0, 1)]
    def combine(g, p, pr):
        slot = lax.rem(g, nb)
        p0 = pr[32*p:32*p+16]; p1 = pr[32*p+16:32*p+32]
        pp = jnp.concatenate([jnp.concatenate([p0, zz], axis=1), jnp.concatenate([zz, p1], axis=1)], axis=0)
        vv = jnp.concatenate([vb[slot, 2*p], vb[slot, 2*p+1]], axis=1)
        o = lax.dot_general(pp, vv, (((1,), (1,)), ((), ())), preferred_element_type=F32)
        ev = []; od = []
        for j in (0, 1):
            oj = o[16*j:16*j+16]
            ev.append(jnp.sum(jnp.where(m_even[:8], oj[:8], 0.0), axis=0, keepdims=True))
            od.append(jnp.sum(jnp.where(m_even[:8], oj[8:], 0.0), axis=0, keepdims=True))
        return ev, od
    def attend(g, nxt):
        rows = pl.ds(pl.multiple_of(g*sb, sb), sb)
        qe = qe_ref[rows, :]
        qo = qo_ref[rows, :]
        sc = []
        for p in range(sb // 2):
            sc += scores(g, p, qe, qo)
            if nxt is not None:
                insert(kb, kt_ref, nxt, p)
        s = jnp.concatenate(sc, axis=0)
        e = jnp.exp(s - jnp.max(s, axis=-1, keepdims=True))
        pr = (e / jnp.sum(e, axis=-1, keepdims=True)).astype(BF)
        oe = []; oo = []
        for p in range(sb // 2):
            ev, od = combine(g, p, pr)
            oe += ev; oo += od
            if nxt is not None:
                insert(vb, vt_ref, nxt, p)
        ae_ref[rows, :] = jnp.concatenate(oe, axis=0)
        ao_ref[rows, :] = jnp.concatenate(oo, axis=0)

    cin(0, 0).wait(); cin(0, 1).wait()
    for p in range(sb // 2):
        insert(kb, kt_ref, jnp.int32(0), p)
        insert(vb, vt_ref, jnp.int32(0), p)
    cout(0, 0).start(); cout(0, 1).start()

    @pl.loop(0, steps - 1)
    def _(g):
        @pl.when((g >= lag) & (g - lag + nb < steps))
        def _():
            cout(g - lag, 0).wait(); cout(g - lag, 1).wait()
            cin(g - lag + nb, 0).start(); cin(g - lag + nb, 1).start()
        cin(g + 1, 0).wait(); cin(g + 1, 1).wait()
        attend(g, g + 1)
        cout(g + 1, 0).start(); cout(g + 1, 1).start()
    attend(jnp.int32(steps - 1), None)

    for c in wcopies[4:]:
        c.wait()
    y = h_ref[...].astype(F32)
    y = y + (jnp.dot(ae_ref[...].astype(BF), woe[...].reshape(dk, -1), preferred_element_type=F32)
             + jnp.dot(ao_ref[...].astype(BF), woo[...].reshape(dk, -1), preferred_element_type=F32))
    y_ref[...] = y
    r = (y * lax.rsqrt(jnp.mean(y*y, axis=-1, keepdims=True) + EPS) * vec_ref[1:2, :]).astype(BF)
    r_ref[...] = r
    lg = lax.dot_general(wr_ref[...], r, (((1,), (1,)), ((), ())), preferred_element_type=F32)
    eid = lax.broadcasted_iota(jnp.int32, lg.shape, 0)
    ids = ids_ref[:, lo:lo+n]
    hot = eid == ids[0:1]
    for j in range(1, ids.shape[0]):
        hot = hot | (eid == ids[j:j+1])
    lg = jnp.where(hot, lg, -jnp.inf)
    e = jnp.where(hot, jnp.exp(lg - jnp.max(lg, axis=0, keepdims=True)), 0.0)
    if later:
        gt_ref[:, :lo] = gp_ref[...]
    gt_ref[:, lo:] = e / jnp.sum(e, axis=0, keepdims=True)
    for j in range(nb):
        cout(steps - nb + j, 0).wait(); cout(steps - nb + j, 1).wait()

def attn_call(arrays, consts, lo, n, prev=None, cfg=(8, 8, 3)):
    hidden, kc, vc, seq_lens, lens_row, ids_t, w_q, w_k, w_v, w_o4, w_rt = arrays
    vec, gain, freq = consts
    d = hidden.shape[1]
    _, dk, t = kc.shape
    nk, _, hd, _ = w_o4.shape
    sb, nb, lag = cfg
    ne = w_rt.shape[0]
    nc = -(-n // 128)
    vm = pl.BlockSpec(memory_space=pltpu.VMEM)
    an = pl.BlockSpec(memory_space=pl.ANY)
    sm = pl.BlockSpec(memory_space=pltpu.SMEM)
    args = [seq_lens, lens_row, ids_t, vec, gain, freq, hidden, w_q, w_k, w_v, w_o4, w_rt, kc, vc]
    specs = [sm, vm, vm, vm, vm, vm, an, an, an, an, an, vm, an, an]
    alias = {}
    if prev is not None:
        args += list(prev)
        specs += [an, an, vm]
        alias = {14: 0, 15: 1}
    frac = n / hidden.shape[0]
    return pl.pallas_call(functools.partial(attn_body, cfg + (lo, prev is not None)),
        out_shape=(jax.ShapeDtypeStruct(kc.shape, BF), jax.ShapeDtypeStruct(vc.shape, BF), jax.ShapeDtypeStruct((n, d), F32),
                   jax.ShapeDtypeStruct((n, d), BF), jax.ShapeDtypeStruct((ne, lo + n), F32)),
        in_specs=specs, out_specs=(an, an, vm, vm, vm), input_output_aliases=alias,
        scratch_shapes=[pltpu.VMEM((nb, sb, dk, t), BF), pltpu.VMEM((nb, sb, dk, t), BF),
            pltpu.VMEM(w_q.shape, BF), pltpu.VMEM(w_k.shape, BF), pltpu.VMEM(w_v.shape, BF),
            pltpu.VMEM((nk, hd, d), BF), pltpu.VMEM((nk, hd, d), BF), pltpu.VMEM((n, d), BF),
            pltpu.VMEM((n, dk), F32), pltpu.VMEM((n, dk), F32), pltpu.VMEM((nc, dk, 128), F32), pltpu.VMEM((nc, dk, 128), F32),
            pltpu.VMEM((n, dk), F32), pltpu.VMEM((n, dk), F32),
            pltpu.SemaphoreType.DMA((2, nb)), pltpu.SemaphoreType.DMA((2, nb)), pltpu.SemaphoreType.DMA((6,))],
        compiler_params=pltpu.CompilerParams(vmem_limit_bytes=60<<20), name="attn",
        cost_estimate=pl.CostEstimate(flops=int(40*10**9*frac), bytes_accessed=int(140*10**6*frac), transcendentals=0),
    )(*args)

def attn_inputs(hidden, k_cache, v_cache, seq_lens, expert_ids, ln_attn, w_q, w_k, w_v, q_gain, k_gain, w_o, ln_moe, w_router):
    n, d = hidden.shape
    t = k_cache.shape[1]; dk = w_k.shape[1]; hd = q_gain.shape[0]; nk = dk // hd
    kc = k_cache.transpose(0, 2, 3, 1).reshape(n, dk, t)
    vc = v_cache.transpose(0, 2, 3, 1).reshape(n, dk, t)
    vec = jnp.stack([ln_attn, ln_moe]).astype(F32)
    gain = jnp.stack([q_gain, k_gain], axis=1).astype(F32)
    freq = jnp.asarray(np.power(np.float32(ROPE_BASE), -np.arange(0, hd, 2).astype(np.float32) / np.float32(hd)).astype(np.float32).reshape(-1, 1))
    arrays = (hidden, kc, vc, seq_lens, seq_lens.reshape(1, n), expert_ids.T, w_q, w_k, w_v, w_o.reshape(nk, 2, hd, d), w_router.T)
    back = lambda z: z.reshape(n, nk, hd, t).transpose(0, 3, 1, 2)
    return arrays, (vec, gain, freq), back


def moe_body(r_ref, gt_ref, y_hbm, wg_own, wu_own, wd_own, wg_par, wu_par, wd_par, out_ref,
             wg, wu, wd, xr, gts, y_ref, act, acc, rbuf, wsem, ysem, agsem_s, agsem_r, gsem_s, gsem_r, rssem_s, rssem_r):
    me = lax.axis_index('ep')
    core = me % 2
    xpos = (me // 2) % 2
    ypos = me // 4
    OWN, X, Y, D = 0, 1, 2, 3
    peers = [None, ypos*4 + (1-xpos)*2 + core, (1-ypos)*4 + xpos*2 + core, (1-ypos)*4 + (1-xpos)*2 + core]
    n_loc = wg_own.shape[0]
    n_exp = 2*n_loc
    hr, hc = acc.shape[3], acc.shape[4]
    ff = wg.shape[2]

    barrier = pltpu.get_barrier_semaphore()
    for p in peers[1:]:
        pl.semaphore_signal(barrier, inc=1, device_id={"ep": p}, device_id_type=pl.DeviceIdType.MESH)

    def wcopy(e, own):
        src = (wg_own, wu_own, wd_own) if own else (wg_par, wu_par, wd_par)
        s = lax.rem(e, n_loc)
        return [pltpu.make_async_copy(a.at[s], b.at[e], wsem.at[i, e]) for i, (a, b) in enumerate(zip(src, (wg, wu, wd)))]
    for e in range(n_exp):
        for c in wcopy(jnp.int32(e), e < n_loc):
            c.start()
    ycopy = pltpu.make_async_copy(y_hbm, y_ref, ysem.at[0])
    ycopy.start()
    pl.semaphore_wait(barrier, 3)

    def remote(src, dst, ss, rs, p):
        return pltpu.make_async_remote_copy(src_ref=src, dst_ref=dst, send_sem=ss, recv_sem=rs,
                                            device_id={"ep": p}, device_id_type=pl.DeviceIdType.MESH)
    ag = {}
    gc = {}
    for b in (D, X, Y):
        rows8 = pl.ds(pl.multiple_of((peers[b] // 2) * n_exp, n_exp), n_exp)
        gc[b] = remote(gt_ref.at[rows8], gts.at[b-1], gsem_s.at[b-1], gsem_r.at[b-1], peers[b])
        gc[b].start()
    for b, h in ((D, 0), (D, 1), (X, 0), (Y, 0), (X, 1), (Y, 1)):
        rows = pl.ds(h*hr, hr)
        ag[b, h] = remote(r_ref.at[rows], xr.at[b-1, rows], agsem_s.at[b-1, h], agsem_r.at[b-1, h], peers[b])
        ag[b, h].start()

    def gates(b):
        if b == OWN:
            return gt_ref[pl.ds(pl.multiple_of((me // 2) * n_exp, n_exp), n_exp), :].T
        return gts[b-1].T

    def compute(load, g8, bs, hs, first=False):
        m = len(bs) * len(hs) * hr
        b0, nb, h0, nh = bs[0], len(bs), hs[0], len(hs)
        lane8 = lax.broadcasted_iota(jnp.int32, (m, n_exp), 1)
        for b in bs:
            for h in hs:
                acc[b, h] = jnp.zeros(acc.shape[2:], F32)
        def step(e, carry):
            if first:
                for c in wcopy(e, True):
                    c.wait()
            gcol = jnp.sum(jnp.where(lane8 == lax.rem(core * n_loc + e, n_exp), g8, 0.0), axis=1, keepdims=True)
            x = load()
            for q in range(2):
                cols = slice(q*ff//2, (q+1)*ff//2)
                g = jnp.dot(x, wg[e, :, cols], preferred_element_type=F32)
                u = jnp.dot(x, wu[e, :, cols], preferred_element_type=F32)
                act[:m, cols] = (jax.nn.silu(g) * u).astype(BF)
            a = act[:m]
            for q in range(4):
                w = hc // 2
                s = (q % 2) * w
                f = jnp.dot(a, wd[e, :, q*w:(q+1)*w], preferred_element_type=F32).astype(BF).astype(F32) * gcol
                i = 0
                for b in bs:
                    for h in hs:
                        acc[b, h, q//2, :, s:s+w] = acc[b, h, q//2, :, s:s+w] + f[i*hr:(i+1)*hr]
                        i += 1
            return carry
        lax.fori_loop(0, n_exp, step, 0)

    def rs(i, h, src, p):
        return remote(src, rbuf.at[i, h], rssem_s.at[i, h], rssem_r.at[i, h], p)
    sent = {}
    def send(i, h, src, b):
        sent[i, h] = rs(i, h, src, peers[b])
        sent[i, h].start()

    compute(lambda: r_ref[...], gates(OWN), (OWN,), (0, 1), first=True)
    gc[D].wait_recv()
    ag[D, 0].wait_recv(); ag[D, 1].wait_recv()
    compute(lambda: xr[D-1], gates(D), (D,), (0, 1))
    for h in (0, 1):
        send(0, h, acc.at[D, h, 0], X)
        send(1, h, acc.at[D, h, 1], Y)
    gc[X].wait_recv()
    gc[Y].wait_recv()
    gx, gy = gates(X), gates(Y)
    for h in (0, 1):
        rows = slice(h*hr, (h+1)*hr)
        ag[X, h].wait_recv(); ag[Y, h].wait_recv()
        compute(lambda: jnp.concatenate([xr[X-1, rows], xr[Y-1, rows]], axis=0), jnp.concatenate([gx[rows], gy[rows]], axis=0), (X, Y), (h,))
        send(2, h, acc.at[X, h, 0], X)
        send(3, h, acc.at[Y, h, 1], Y)
        sent[1, h].wait_recv()
        acc[X, h, 1] = acc[X, h, 1] + rbuf[1, h]
        send(4, h, acc.at[X, h, 1], X)
        sent[0, h].wait_recv()
        acc[Y, h, 0] = acc[Y, h, 0] + rbuf[0, h]
        send(5, h, acc.at[Y, h, 0], Y)
    ycopy.wait()
    for h in (0, 1):
        rows = slice(h*hr, (h+1)*hr)
        sent[2, h].wait_recv()
        sent[3, h].wait_recv()
        acc[OWN, h, 0] = y_ref[rows, :hc] + (acc[OWN, h, 0] + rbuf[2, h])
        acc[OWN, h, 1] = y_ref[rows, hc:] + (acc[OWN, h, 1] + rbuf[3, h])
        sent[5, h].wait_recv()
        out_ref[rows, :hc] = (acc[OWN, h, 0] + rbuf[5, h]).astype(out_ref.dtype)
        sent[4, h].wait_recv()
        out_ref[rows, hc:] = (acc[OWN, h, 1] + rbuf[4, h]).astype(out_ref.dtype)
    for c in (*gc.values(), *ag.values(), *sent.values()):
        c.wait_send()

def moe_call(r, gt, y, w_gate, w_up, w_down, wg_p, wu_p, wd_p):
    n, d = r.shape
    nl, _, ff = w_gate.shape
    vm = pl.BlockSpec(memory_space=pltpu.VMEM)
    an = pl.BlockSpec(memory_space=pl.ANY)
    dma = pltpu.SemaphoreType.DMA
    return pl.pallas_call(moe_body,
        out_shape=jax.ShapeDtypeStruct((n, d), BF),
        in_specs=[vm, vm] + [an]*7, out_specs=vm,
        scratch_shapes=[pltpu.VMEM((2*nl, d, ff), BF), pltpu.VMEM((2*nl, d, ff), BF), pltpu.VMEM((2*nl, ff, d), BF),
            pltpu.VMEM((3, n, d), BF), pltpu.VMEM((3, 2*nl, n), F32), pltpu.VMEM((n, d), F32), pltpu.VMEM((n, ff), BF),
            pltpu.VMEM((4, 2, 2, n//2, d//2), F32), pltpu.VMEM((6, 2, n//2, d//2), F32),
            dma((3, 2*nl)), dma((1,)), dma((3, 2)), dma((3, 2)), dma((3,)), dma((3,)), dma((6, 2)), dma((6, 2))],
        compiler_params=pltpu.CompilerParams(vmem_limit_bytes=60<<20, collective_id=1, has_side_effects=True), name="moe",
        cost_estimate=pl.CostEstimate(flops=26*10**9, bytes_accessed=30*10**6, transcendentals=0),
    )(r, gt, y, w_gate, w_up, w_down, wg_p, wu_p, wd_p)


def solution(mesh):
    n_group = mesh.shape['ep']
    row_spec = P(('dp', 'ep'), None)
    cache_spec = P(('dp', 'ep'), None, None, None)
    len_spec = P(('dp', 'ep'))
    rep_vec = P(None)
    rep_mat = P(None, None)
    exp_spec = P('ep', None, None)
    swap = [(i, i + 1 - 2 * (i % 2)) for i in range(n_group)]

    def local_step(hidden, k_cache, v_cache, seq_lens, expert_ids, ln_attn, w_q, w_k, w_v, q_gain, k_gain, w_o, ln_moe, w_router, w_gate, w_up, w_down):
        wg_p = lax.ppermute(w_gate, 'ep', swap)
        wu_p = lax.ppermute(w_up, 'ep', swap)
        wd_p = lax.ppermute(w_down, 'ep', swap)
        arrays, consts, back = attn_inputs(hidden, k_cache, v_cache, seq_lens, expert_ids, ln_attn, w_q, w_k, w_v, q_gain, k_gain, w_o, ln_moe, w_router)
        ko, vo, y, r, gt = attn_call(arrays, consts, 0, hidden.shape[0])
        out = moe_call(r, gt, y, w_gate, w_up, w_down, wg_p, wu_p, wd_p)
        return out, back(ko), back(vo)

    return jax.shard_map(local_step, mesh=mesh, in_specs=(row_spec, cache_spec, cache_spec, len_spec, row_spec, rep_vec, rep_mat, rep_mat, rep_mat, rep_vec, rep_vec, rep_mat, rep_vec, rep_mat, exp_spec, exp_spec, exp_spec), out_specs=(row_spec, cache_spec, cache_spec), check_vma=False)
```

```python
import functools
import numpy as np
import jax, jax.numpy as jnp
from jax import lax
from jax.experimental import pallas as pl
from jax.experimental.pallas import tpu as pltpu
from jax.sharding import PartitionSpec as P
EPS=1e-6; ROPE_BASE=1e6
F32=jnp.float32; BF=jnp.bfloat16

def attn_body(cfg, lens_s, ids_ref, lnm_ref, h_hbm, wo_hbm, wr_ref, k_hbm, v_hbm, *refs):
    sb, nb, lag, lo, n, first, last = cfg
    n_kv, hd, dk = 8, 64, 512
    if first:
        lens_ref, lna_ref, qg_ref, kg_ref, freq_ref, wq_hbm, wk_hbm, wv_hbm = refs[:8]
        refs = refs[8:]
    else:
        qe_ref, qo_ref, kt_ref, vt_ref, _, _, gp_ref = refs[:7]
        refs = refs[7:]
    ko_hbm, vo_hbm, y_ref, r_ref, gt_ref = refs[:5]
    refs = refs[5:]
    if first and not last:
        qeb_ref, qob_ref, ktb_ref, vtb_ref = refs[:4]
        refs = refs[4:]
    kb, vb, woe, woo, h_ref, ae_ref, ao_ref, isem, osem, wsem = refs[:10]
    if first:
        qe_ref, qo_ref, kt_ref, vt_ref, wq, wk, wv, qsem = refs[10:]
    steps = n // sb
    per = 128 // sb
    def cin(g, which):
        s = lax.rem(g, nb)
        r, b = ((k_hbm, kb), (v_hbm, vb))[which]
        return pltpu.make_async_copy(r.at[pl.ds(lo + g*sb, sb)], b.at[s], isem.at[which, s])
    def cout(g, which):
        s = lax.rem(g, nb)
        r, b = ((ko_hbm, kb), (vo_hbm, vb))[which]
        return pltpu.make_async_copy(b.at[s], r.at[pl.ds(lo + g*sb, sb)], osem.at[which, s])
    late = [pltpu.make_async_copy(a, b, wsem.at[i]) for i, (a, b) in enumerate(((wo_hbm.at[:, 0], woe), (wo_hbm.at[:, 1], woo)))]
    early = [pltpu.make_async_copy(h_hbm if first else h_hbm.at[pl.ds(lo, n)], h_ref, wsem.at[2])]
    if first:
        early += [pltpu.make_async_copy(a, b, qsem.at[i]) for i, (a, b) in enumerate(((wq_hbm, wq), (wk_hbm, wk), (wv_hbm, wv)))]
    for c in early:
        c.start()
    if first:
        cin(0, 0).start(); cin(0, 1).start()
        for c in early:
            c.wait()
    for g in range(*((1, nb) if first else (0, 2))):
        cin(g, 0).start(); cin(g, 1).start()
    for c in late:
        c.start()
    if first:
        na = h_ref.shape[0]
        h = h_ref[...].astype(F32)
        x = (h * lax.rsqrt(jnp.mean(h*h, axis=-1, keepdims=True) + EPS) * lna_ref[...].astype(F32)[None, :]).astype(BF)
        ang = freq_ref[...] * lens_ref[...].astype(F32)[None, :]
        cos_v = jnp.cos(ang)[None]; sin_v = jnp.sin(ang)[None]
        half = hd // 2
        eye = lax.broadcasted_iota(jnp.int32, (hd, hd), 0) == lax.broadcasted_iota(jnp.int32, (hd, hd), 1)
        def norm_rope(w_ref, g_ref):
            gain = jnp.sum(jnp.where(eye, g_ref[...].astype(F32)[None, :], 0.0), axis=1, keepdims=True)
            p = jnp.dot(x, w_ref[...], preferred_element_type=F32)
            p = p.T.reshape(-1, hd, na)
            p = p * lax.rsqrt(jnp.mean(p*p, axis=1, keepdims=True) + EPS) * gain[None]
            lo_, hi = p[:, :half], p[:, half:]
            return jnp.concatenate([lo_*cos_v - hi*sin_v, hi*cos_v + lo_*sin_v], axis=1)
        q = norm_rope(wq, qg_ref)
        q = q.reshape(n_kv, 2, hd, na)
        qe = q[:, 0].reshape(dk, na).T
        qo = q[:, 1].reshape(dk, na).T
        qe_ref[...] = qe[:n]
        qo_ref[...] = qo[:n]
        k = norm_rope(wk, kg_ref).reshape(dk, na).astype(BF).astype(F32)
        v = jnp.dot(x, wv[...], preferred_element_type=F32).T.astype(BF).astype(F32)
        for c in range(n // 128):
            kt_ref[c] = k[:, 128*c:128*c+128]
            vt_ref[c] = v[:, 128*c:128*c+128]
        if not last:
            qeb_ref[...] = qe[n:]
            qob_ref[...] = qo[n:]
            for c in range((na - n) // 128):
                ktb_ref[c] = k[:, n+128*c:n+128*c+128]
                vtb_ref[c] = v[:, n+128*c:n+128*c+128]
    else:
        for c in early:
            c.wait()

    lane = lax.broadcasted_iota(jnp.int32, (1, 128), 1)
    row = lax.broadcasted_iota(jnp.int32, (16, dk), 0)
    col = lax.broadcasted_iota(jnp.int32, (16, dk), 1) // hd
    m_even = row == col
    m_odd = row == col + n_kv

    zz = jnp.zeros((16, 128), BF)
    def fresh(t_ref, g, i):
        ln = lens_s[lo + g*sb + i]
        col = pltpu.roll(t_ref[g // per], lax.rem(ln - (lax.rem(g, per) * sb + i) + 128, 128), 1).astype(BF)
        return lane == ln, col
    def insert(buf, t_ref, g, p):
        slot = lax.rem(g, nb)
        for i in (2*p, 2*p+1):
            hit, col = fresh(t_ref, g, i)
            buf[slot, i] = jnp.where(hit, col, buf[slot, i])
    def scores(g, p, qe, qo):
        slot = lax.rem(g, nb)
        qs = [jnp.where(m_even, qe[i:i+1], jnp.where(m_odd, qo[i:i+1], 0.0)).astype(BF) for i in (2*p, 2*p+1)]
        ks = jnp.concatenate([kb[slot, 2*p], kb[slot, 2*p+1]], axis=1)
        s = jnp.dot(jnp.concatenate(qs, axis=0), ks, preferred_element_type=F32)
        return [jnp.where(lane <= lens_s[lo + g*sb + 2*p + j], s[16*j:16*j+16, 128*j:128*j+128] * (hd ** -0.5), -1e30) for j in (0, 1)]
    def combine(g, p, pr):
        slot = lax.rem(g, nb)
        p0 = pr[32*p:32*p+16]; p1 = pr[32*p+16:32*p+32]
        pp = jnp.concatenate([jnp.concatenate([p0, zz], axis=1), jnp.concatenate([zz, p1], axis=1)], axis=0)
        vv = jnp.concatenate([vb[slot, 2*p], vb[slot, 2*p+1]], axis=1)
        o = lax.dot_general(pp, vv, (((1,), (1,)), ((), ())), preferred_element_type=F32)
        ev = []; od = []
        for j in (0, 1):
            oj = o[16*j:16*j+16]
            ev.append(jnp.sum(jnp.where(m_even[:8], oj[:8], 0.0), axis=0, keepdims=True))
            od.append(jnp.sum(jnp.where(m_even[:8], oj[8:], 0.0), axis=0, keepdims=True))
        return ev, od
    def attend(g, nxt):
        rows = pl.ds(pl.multiple_of(g*sb, sb), sb)
        qe = qe_ref[rows, :]
        qo = qo_ref[rows, :]
        sc = []
        for p in range(sb // 2):
            sc += scores(g, p, qe, qo)
        s = jnp.concatenate(sc, axis=0)
        e = jnp.exp(s - jnp.max(s, axis=-1, keepdims=True))
        pr = (e / jnp.sum(e, axis=-1, keepdims=True)).astype(BF)
        oe = []; oo = []
        for p in range(sb // 2):
            ev, od = combine(g, p, pr)
            oe += ev; oo += od
            if nxt is not None:
                insert(kb, kt_ref, nxt, p)
                insert(vb, vt_ref, nxt, p)
        ae_ref[rows, :] = jnp.concatenate(oe, axis=0)
        ao_ref[rows, :] = jnp.concatenate(oo, axis=0)

    cin(0, 0).wait(); cin(0, 1).wait()
    for p in range(sb // 2):
        insert(kb, kt_ref, jnp.int32(0), p)
        insert(vb, vt_ref, jnp.int32(0), p)
    cout(0, 0).start(); cout(0, 1).start()
    for g in range(nb if first else 2, nb):
        cin(g, 0).start(); cin(g, 1).start()

    @pl.loop(0, steps - 1)
    def _(g):
        @pl.when((g >= lag) & (g - lag + nb < steps))
        def _():
            cout(g - lag, 0).wait(); cout(g - lag, 1).wait()
            cin(g - lag + nb, 0).start(); cin(g - lag + nb, 1).start()
        cin(g + 1, 0).wait(); cin(g + 1, 1).wait()
        attend(g, g + 1)
        cout(g + 1, 0).start(); cout(g + 1, 1).start()
    attend(jnp.int32(steps - 1), None)

    for c in late:
        c.wait()
    y = h_ref[:n].astype(F32)
    y = y + (jnp.dot(ae_ref[...].astype(BF), woe[...].reshape(dk, -1), preferred_element_type=F32)
             + jnp.dot(ao_ref[...].astype(BF), woo[...].reshape(dk, -1), preferred_element_type=F32))
    y_ref[...] = y
    r = (y * lax.rsqrt(jnp.mean(y*y, axis=-1, keepdims=True) + EPS) * lnm_ref[...].astype(F32)[None, :]).astype(BF)
    r_ref[...] = r
    lg = lax.dot_general(wr_ref[...], r, (((1,), (1,)), ((), ())), preferred_element_type=F32)
    eid = lax.broadcasted_iota(jnp.int32, lg.shape, 0)
    ids = ids_ref[:, lo:lo+n]
    hot = eid == ids[0:1]
    for j in range(1, ids.shape[0]):
        hot = hot | (eid == ids[j:j+1])
    lg = jnp.where(hot, lg, -jnp.inf)
    e = jnp.where(hot, jnp.exp(lg - jnp.max(lg, axis=0, keepdims=True)), 0.0)
    if not first:
        gt_ref[:, :lo] = gp_ref[...]
    gt_ref[:, lo:] = e / jnp.sum(e, axis=0, keepdims=True)
    for j in range(nb):
        cout(steps - nb + j, 0).wait(); cout(steps - nb + j, 1).wait()

def attn_call(hidden, kc, vc, seq_lens, expert_ids, ln_attn, w_q, w_k, w_v, q_gain, k_gain, w_o, ln_moe, w_router, lo, n, prev=None, cfg=(8, 8, 3)):
    ntot, d = hidden.shape
    _, dk, t = kc.shape
    hd = q_gain.shape[0]
    nk = dk // hd
    sb, nb, lag = cfg
    ne = w_router.shape[1]
    first, last = lo == 0, lo + n == ntot
    vm = pl.BlockSpec(memory_space=pltpu.VMEM)
    an = pl.BlockSpec(memory_space=pl.ANY)
    sm = pl.BlockSpec(memory_space=pltpu.SMEM)
    args = [seq_lens, expert_ids.T, ln_moe, hidden, w_o.reshape(nk, 2, hd, d), w_router.T, kc, vc]
    specs = [sm, vm, vm, an, an, vm, an, an]
    alias = {}
    shape = jax.ShapeDtypeStruct
    outs = [shape(kc.shape, BF), shape(vc.shape, BF), shape((n, d), F32), shape((n, d), BF), shape((ne, lo + n), F32)]
    ospecs = [an, an, vm, vm, vm]
    dma = pltpu.SemaphoreType.DMA
    scratch = [pltpu.VMEM((nb, sb, dk, t), BF), pltpu.VMEM((nb, sb, dk, t), BF), pltpu.VMEM((nk, hd, d), BF), pltpu.VMEM((nk, hd, d), BF),
               pltpu.VMEM((ntot if first else n, d), BF), pltpu.VMEM((n, dk), F32), pltpu.VMEM((n, dk), F32), dma((2, nb)), dma((2, nb)), dma((3,))]
    if first:
        freq = np.power(np.float32(ROPE_BASE), -np.arange(0, hd, 2).astype(np.float32) / np.float32(hd)).astype(np.float32).reshape(-1, 1)
        args += [seq_lens, ln_attn, q_gain, k_gain, jnp.asarray(freq), w_q, w_k, w_v]
        specs += [vm]*5 + [an]*3
        scratch += [pltpu.VMEM((n, dk), F32), pltpu.VMEM((n, dk), F32), pltpu.VMEM((n//128, dk, 128), F32), pltpu.VMEM((n//128, dk, 128), F32),
                    pltpu.VMEM(w_q.shape, BF), pltpu.VMEM(w_k.shape, BF), pltpu.VMEM(w_v.shape, BF), dma((3,))]
        if not last:
            m = ntot - n
            outs += [shape((m, dk), F32), shape((m, dk), F32), shape((m//128, dk, 128), F32), shape((m//128, dk, 128), F32)]
            ospecs += [vm]*4
    else:
        args += list(prev)
        specs += [vm]*4 + [an, an, vm]
        alias = {12: 0, 13: 1}
    frac = n / ntot
    return pl.pallas_call(functools.partial(attn_body, cfg + (lo, n, first, last)), out_shape=outs, in_specs=specs, out_specs=ospecs,
        input_output_aliases=alias, scratch_shapes=scratch,
        compiler_params=pltpu.CompilerParams(vmem_limit_bytes=67043328), name="attn",
        cost_estimate=pl.CostEstimate(flops=int(40*10**9*frac), bytes_accessed=int(140*10**6*frac), transcendentals=0),
    )(*args)

def cache_views(c):
    n, t, nk, hd = c.shape
    return c.transpose(0, 2, 3, 1).reshape(n, nk*hd, t), lambda z: z.reshape(n, nk, hd, t).transpose(0, 3, 1, 2)


def moe_body(ra_hbm, rx_hbm, ry_hbm, rd_hbm, rb_hbm, gt_hbm, ya_hbm, yb_hbm, wg_own, wu_own, wd_own, wg_par, wu_par, wd_par, out_ref,
             wg, wu, wd, xa, xb, xr, gt_ref, gts, y_ref, act, acc, rbuf, wsem, xsem, ysem, agsem_s, agsem_r, gsem_s, gsem_r, rssem_s, rssem_r):
    me = lax.axis_index('ep')
    core = me % 2
    xpos = (me // 2) % 2
    ypos = me // 4
    OWN, X, Y, D = 0, 1, 2, 3
    peers = [None, ypos*4 + (1-xpos)*2 + core, (1-ypos)*4 + xpos*2 + core, (1-ypos)*4 + (1-xpos)*2 + core]
    n_loc = wg_own.shape[0]
    n_exp = 2*n_loc
    hr, hc = acc.shape[3], acc.shape[4]
    ff = wg.shape[2]

    barrier = pltpu.get_barrier_semaphore()
    for p in peers[1:]:
        pl.semaphore_signal(barrier, inc=1, device_id={"ep": p}, device_id_type=pl.DeviceIdType.MESH)

    def wcopy(e, own):
        src = (wg_own, wu_own, wd_own) if own else (wg_par, wu_par, wd_par)
        s = lax.rem(e, n_loc)
        return [pltpu.make_async_copy(a.at[s], b.at[e], wsem.at[i, e]) for i, (a, b) in enumerate(zip(src, (wg, wu, wd)))]
    own = [pltpu.make_async_copy(rb_hbm, xb, xsem.at[4]), pltpu.make_async_copy(gt_hbm, gt_ref, xsem.at[5])]
    for c in own:
        c.start()
    heads = [pltpu.make_async_copy(a, xa.at[b], xsem.at[b]) for b, a in enumerate((ra_hbm, rx_hbm, ry_hbm, rd_hbm))]
    heads[D].start()
    for c in wcopy(jnp.int32(0), True):
        c.start()
    for b in (X, Y, OWN):
        heads[b].start()
    ahead = 2
    for e in range(1, ahead):
        for c in wcopy(jnp.int32(e), True):
            c.start()
    ycopy = [pltpu.make_async_copy(a, y_ref.at[pl.ds(h*hr, hr)], ysem.at[h]) for h, a in enumerate((ya_hbm, yb_hbm))]
    for c in ycopy:
        c.start()
    for c in own:
        c.wait()
    pl.semaphore_wait(barrier, 3)

    def remote(src, dst, ss, rs, p):
        return pltpu.make_async_remote_copy(src_ref=src, dst_ref=dst, send_sem=ss, recv_sem=rs,
                                            device_id={"ep": p}, device_id_type=pl.DeviceIdType.MESH)
    ag = {}
    gc = {}
    for b in (D, X, Y):
        rows8 = pl.ds(pl.multiple_of((peers[b] // 2) * n_exp, n_exp), n_exp)
        gc[b] = remote(gt_ref.at[rows8], gts.at[b-1], gsem_s.at[b-1], gsem_r.at[b-1], peers[b])
        gc[b].start()
    for b in (D, X, Y):
        ag[b] = remote(xb, xr.at[b-1], agsem_s.at[b-1], agsem_r.at[b-1], peers[b])
        ag[b].start()

    def gates(b):
        if b == OWN:
            return gt_ref[pl.ds(pl.multiple_of((me // 2) * n_exp, n_exp), n_exp), :].T
        return gts[b-1].T

    def compute(load, g8, bs, hs, first=False):
        m = len(bs) * len(hs) * hr
        b0, nb, h0, nh = bs[0], len(bs), hs[0], len(hs)
        lane8 = lax.broadcasted_iota(jnp.int32, (m, n_exp), 1)
        for b in bs:
            for h in hs:
                acc[b, h] = jnp.zeros(acc.shape[2:], F32)
        def step(e, carry):
            if first:
                for c in wcopy(e, True):
                    c.wait()
                @pl.when(e + ahead < n_loc)
                def _():
                    for c in wcopy(e + ahead, True):
                        c.start()
                @pl.when((e + ahead >= n_loc) & (e + ahead < n_exp))
                def _():
                    for c in wcopy(e + ahead, False):
                        c.start()
            gcol = jnp.sum(jnp.where(lane8 == lax.rem(core * n_loc + e, n_exp), g8, 0.0), axis=1, keepdims=True)
            x = load()
            for q in range(2):
                cols = slice(q*ff//2, (q+1)*ff//2)
                g = jnp.dot(x, wg[e, :, cols], preferred_element_type=F32)
                u = jnp.dot(x, wu[e, :, cols], preferred_element_type=F32)
                act[:m, cols] = (jax.nn.silu(g) * u).astype(BF)
            a = act[:m]
            for q in range(4):
                w = hc // 2
                s = (q % 2) * w
                f = jnp.dot(a, wd[e, :, q*w:(q+1)*w], preferred_element_type=F32).astype(BF).astype(F32) * gcol
                i = 0
                for b in bs:
                    for h in hs:
                        acc[b, h, q//2, :, s:s+w] = acc[b, h, q//2, :, s:s+w] + f[i*hr:(i+1)*hr]
                        i += 1
            return carry
        lax.fori_loop(0, n_exp, step, 0)

    def rs(i, h, src, p):
        return remote(src, rbuf.at[i, h], rssem_s.at[i, h], rssem_r.at[i, h], p)
    sent = {}
    def send(i, h, src, b):
        sent[i, h] = rs(i, h, src, peers[b])
        sent[i, h].start()

    def diagonal(h):
        rows = slice(h*hr, (h+1)*hr)
        compute(lambda: xa[D] if h == 0 else xr[D-1], gates(D)[rows], (D,), (h,), first=h == 0)
        send(0, h, acc.at[D, h, 0], X)
        send(1, h, acc.at[D, h, 1], Y)
    def neighbours(h):
        rows = slice(h*hr, (h+1)*hr)
        compute(lambda: (xa[X:D] if h == 0 else xr[X-1:D-1]).reshape(2*hr, -1), jnp.concatenate([gates(X)[rows], gates(Y)[rows]], axis=0), (X, Y), (h,))
        send(2, h, acc.at[X, h, 0], X)
        send(3, h, acc.at[Y, h, 1], Y)
    def pass_on(h):
        sent[1, h].wait_recv()
        acc[X, h, 1] = acc[X, h, 1] + rbuf[1, h]
        send(4, h, acc.at[X, h, 1], X)
        sent[0, h].wait_recv()
        acc[Y, h, 0] = acc[Y, h, 0] + rbuf[0, h]
        send(5, h, acc.at[Y, h, 0], Y)
    heads[D].wait()
    gc[D].wait_recv()
    diagonal(0)
    heads[X].wait()
    heads[Y].wait()
    gc[X].wait_recv(); gc[Y].wait_recv()
    neighbours(0)
    ag[D].wait_recv()
    diagonal(1)
    pass_on(0)
    ag[X].wait_recv(); ag[Y].wait_recv()
    neighbours(1)
    heads[OWN].wait()
    compute(lambda: jnp.concatenate([xa[OWN], xb[...]], axis=0), gates(OWN), (OWN,), (0, 1))
    pass_on(1)
    for c in ycopy:
        c.wait()
    for h in (0, 1):
        rows = slice(h*hr, (h+1)*hr)
        sent[2, h].wait_recv()
        sent[3, h].wait_recv()
        acc[OWN, h, 0] = y_ref[rows, :hc] + (acc[OWN, h, 0] + rbuf[2, h])
        acc[OWN, h, 1] = y_ref[rows, hc:] + (acc[OWN, h, 1] + rbuf[3, h])
        sent[5, h].wait_recv()
        out_ref[rows, :hc] = (acc[OWN, h, 0] + rbuf[5, h]).astype(out_ref.dtype)
        sent[4, h].wait_recv()
        out_ref[rows, hc:] = (acc[OWN, h, 1] + rbuf[4, h]).astype(out_ref.dtype)
    for c in (*gc.values(), *ag.values(), *sent.values()):
        c.wait_send()

def moe_call(ra, rx, ry, rd, rb, gt, ya, yb, w_gate, w_up, w_down, wg_p, wu_p, wd_p):
    n, d = 2*ra.shape[0], ra.shape[1]
    nl, _, ff = w_gate.shape
    vm = pl.BlockSpec(memory_space=pltpu.VMEM)
    an = pl.BlockSpec(memory_space=pl.ANY)
    dma = pltpu.SemaphoreType.DMA
    return pl.pallas_call(moe_body,
        out_shape=jax.ShapeDtypeStruct((n, d), BF),
        in_specs=[an]*14, out_specs=vm,
        scratch_shapes=[pltpu.VMEM((2*nl, d, ff), BF), pltpu.VMEM((2*nl, d, ff), BF), pltpu.VMEM((2*nl, ff, d), BF),
            pltpu.VMEM((4, n//2, d), BF), pltpu.VMEM((n//2, d), BF), pltpu.VMEM((3, n//2, d), BF), pltpu.VMEM(gt.shape, F32), pltpu.VMEM((3, 2*nl, n), F32), pltpu.VMEM((n, d), F32), pltpu.VMEM((n, ff), BF),
            pltpu.VMEM((4, 2, 2, n//2, d//2), F32), pltpu.VMEM((6, 2, n//2, d//2), F32),
            dma((3, 2*nl)), dma((6,)), dma((2,)), dma((3,)), dma((3,)), dma((3,)), dma((3,)), dma((6, 2)), dma((6, 2))],
        compiler_params=pltpu.CompilerParams(vmem_limit_bytes=67043328, collective_id=1, has_side_effects=True), name="moe",
        cost_estimate=pl.CostEstimate(flops=26*10**9, bytes_accessed=30*10**6, transcendentals=0),
    )(ra, rx, ry, rd, rb, gt, ya, yb, w_gate, w_up, w_down, wg_p, wu_p, wd_p)


def solution(mesh):
    n_group = mesh.shape['ep']
    row_spec = P(('dp', 'ep'), None)
    cache_spec = P(('dp', 'ep'), None, None, None)
    len_spec = P(('dp', 'ep'))
    rep_vec = P(None)
    rep_mat = P(None, None)
    exp_spec = P('ep', None, None)
    swap = [(i, i + 1 - 2 * (i % 2)) for i in range(n_group)]
    flip = lambda k: [(i, i ^ k) for i in range(n_group)]

    def local_step(hidden, k_cache, v_cache, seq_lens, expert_ids, ln_attn, w_q, w_k, w_v, q_gain, k_gain, w_o, ln_moe, w_router, w_gate, w_up, w_down):
        wg_p = lax.ppermute(w_gate, 'ep', swap)
        wu_p = lax.ppermute(w_up, 'ep', swap)
        wd_p = lax.ppermute(w_down, 'ep', swap)
        n = hidden.shape[0]
        na = n // 2
        kc, back = cache_views(k_cache)
        vc, _ = cache_views(v_cache)
        args = (hidden, kc, vc, seq_lens, expert_ids, ln_attn, w_q, w_k, w_v, q_gain, k_gain, w_o, ln_moe, w_router)
        ko, vo, ya, ra, gt, *mid = attn_call(*args, 0, na)
        rd = lax.ppermute(ra, 'ep', flip(6))
        rx = lax.ppermute(ra, 'ep', flip(2))
        ry = lax.ppermute(ra, 'ep', flip(4))
        ko, vo, yb, rb, gt = attn_call(*args, na, n - na, prev=(*mid, ko, vo, gt))
        out = moe_call(ra, rx, ry, rd, rb, gt, ya, yb, w_gate, w_up, w_down, wg_p, wu_p, wd_p)
        return out, back(ko), back(vo)

    return jax.shard_map(local_step, mesh=mesh, in_specs=(row_spec, cache_spec, cache_spec, len_spec, row_spec, rep_vec, rep_mat, rep_mat, rep_mat, rep_vec, rep_vec, rep_mat, rep_vec, rep_mat, exp_spec, exp_spec, exp_spec), out_specs=(row_spec, cache_spec, cache_spec), check_vma=False)
```

```python
import functools
import numpy as np
import jax, jax.numpy as jnp
from jax import lax
from jax.experimental import pallas as pl
from jax.experimental.pallas import tpu as pltpu
from jax.sharding import PartitionSpec as P
EPS=1e-6; ROPE_BASE=1e6
F32=jnp.float32; BF=jnp.bfloat16

def attn_body(cfg, lens_hbm, ids_hbm, lnm_hbm, h_hbm, wo_hbm, wr_hbm, k_hbm, v_hbm, *refs):
    sb, nb, lag, lo, n, first, last = cfg
    n_kv, hd, dk = 8, 64, 512
    if first:
        lna_hbm, qg_hbm, kg_hbm, freq_hbm, wq_hbm, wk_hbm, wv_hbm = refs[:7]
        refs = refs[7:]
    else:
        qe_ref, qo_ref, kt_ref, vt_ref, _, _, gp_ref = refs[:7]
        refs = refs[7:]
    ko_hbm, vo_hbm, y_ref, r_ref, gt_ref = refs[:5]
    refs = refs[5:]
    if first and not last:
        qeb_ref, qob_ref, ktb_ref, vtb_ref = refs[:4]
        refs = refs[4:]
    kb, vb, woe, woo, h_ref, ae_ref, ao_ref, lens_s, ids_ref, lnm_ref, wr_ref, isem, osem, wsem = refs[:14]
    if first:
        qe_ref, qo_ref, kt_ref, vt_ref, wq, wk, wv, lens_ref, lna_ref, qg_ref, kg_ref, freq_ref, qsem = refs[14:]
    steps = n // sb
    per = 128 // sb
    def cin(g, which):
        s = lax.rem(g, nb)
        r, b = ((k_hbm, kb), (v_hbm, vb))[which]
        return pltpu.make_async_copy(r.at[pl.ds(lo + g*sb, sb)], b.at[s], isem.at[which, s])
    def cout(g, which):
        s = lax.rem(g, nb)
        r, b = ((ko_hbm, kb), (vo_hbm, vb))[which]
        return pltpu.make_async_copy(b.at[s], r.at[pl.ds(lo + g*sb, sb)], osem.at[which, s])
    late = [pltpu.make_async_copy(a, b, wsem.at[i]) for i, (a, b) in enumerate(((wo_hbm.at[:, 0], woe), (wo_hbm.at[:, 1], woo), (ids_hbm, ids_ref), (lnm_hbm, lnm_ref), (wr_hbm, wr_ref)))]
    early = [pltpu.make_async_copy(h_hbm if first else h_hbm.at[pl.ds(lo, n)], h_ref, wsem.at[5]), pltpu.make_async_copy(lens_hbm, lens_s, wsem.at[6])]
    if first:
        early += [pltpu.make_async_copy(a, b, qsem.at[i]) for i, (a, b) in enumerate(((lens_hbm, lens_ref), (lna_hbm, lna_ref), (qg_hbm, qg_ref), (kg_hbm, kg_ref), (freq_hbm, freq_ref), (wq_hbm, wq), (wk_hbm, wk), (wv_hbm, wv)))]
    for c in early:
        c.start()
    if first:
        cin(0, 0).start(); cin(0, 1).start()
        for c in early:
            c.wait()
    for g in range(*((1, nb) if first else (0, 2))):
        cin(g, 0).start(); cin(g, 1).start()
    for c in late:
        c.start()
    if first:
        na = h_ref.shape[0]
        h = h_ref[...].astype(F32)
        x = (h * lax.rsqrt(jnp.mean(h*h, axis=-1, keepdims=True) + EPS) * lna_ref[...].astype(F32)[None, :]).astype(BF)
        ang = freq_ref[...] * lens_ref[...].astype(F32)[None, :]
        cos_v = jnp.cos(ang)[None]; sin_v = jnp.sin(ang)[None]
        half = hd // 2
        eye = lax.broadcasted_iota(jnp.int32, (hd, hd), 0) == lax.broadcasted_iota(jnp.int32, (hd, hd), 1)
        def norm_rope(w_ref, g_ref):
            gain = jnp.sum(jnp.where(eye, g_ref[...].astype(F32)[None, :], 0.0), axis=1, keepdims=True)
            p = jnp.dot(x, w_ref[...], preferred_element_type=F32)
            p = p.T.reshape(-1, hd, na)
            p = p * lax.rsqrt(jnp.mean(p*p, axis=1, keepdims=True) + EPS) * gain[None]
            lo_, hi = p[:, :half], p[:, half:]
            return jnp.concatenate([lo_*cos_v - hi*sin_v, hi*cos_v + lo_*sin_v], axis=1)
        q = norm_rope(wq, qg_ref)
        q = q.reshape(n_kv, 2, hd, na)
        qe = q[:, 0].reshape(dk, na).T
        qo = q[:, 1].reshape(dk, na).T
        qe_ref[...] = qe[:n]
        qo_ref[...] = qo[:n]
        k = norm_rope(wk, kg_ref).reshape(dk, na).astype(BF).astype(F32)
        v = jnp.dot(x, wv[...], preferred_element_type=F32).T.astype(BF).astype(F32)
        for c in range(n // 128):
            kt_ref[c] = k[:, 128*c:128*c+128]
            vt_ref[c] = v[:, 128*c:128*c+128]
        if not last:
            qeb_ref[...] = qe[n:]
            qob_ref[...] = qo[n:]
            for c in range((na - n) // 128):
                ktb_ref[c] = k[:, n+128*c:n+128*c+128]
                vtb_ref[c] = v[:, n+128*c:n+128*c+128]
    else:
        for c in early:
            c.wait()

    lane = lax.broadcasted_iota(jnp.int32, (1, 128), 1)
    row = lax.broadcasted_iota(jnp.int32, (16, dk), 0)
    col = lax.broadcasted_iota(jnp.int32, (16, dk), 1) // hd
    m_even = row == col
    m_odd = row == col + n_kv

    zz = jnp.zeros((16, 128), BF)
    def fresh(t_ref, g, i):
        ln = lens_s[lo + g*sb + i]
        col = pltpu.roll(t_ref[g // per], lax.rem(ln - (lax.rem(g, per) * sb + i) + 128, 128), 1).astype(BF)
        return lane == ln, col
    def insert(buf, t_ref, g, p):
        slot = lax.rem(g, nb)
        for i in (2*p, 2*p+1):
            hit, col = fresh(t_ref, g, i)
            buf[slot, i] = jnp.where(hit, col, buf[slot, i])
    def scores(g, p, qe, qo):
        slot = lax.rem(g, nb)
        qs = [jnp.where(m_even, qe[i:i+1], jnp.where(m_odd, qo[i:i+1], 0.0)).astype(BF) for i in (2*p, 2*p+1)]
        ks = jnp.concatenate([kb[slot, 2*p], kb[slot, 2*p+1]], axis=1)
        s = jnp.dot(jnp.concatenate(qs, axis=0), ks, preferred_element_type=F32)
        return [jnp.where(lane <= lens_s[lo + g*sb + 2*p + j], s[16*j:16*j+16, 128*j:128*j+128] * (hd ** -0.5), -1e30) for j in (0, 1)]
    def combine(g, p, pr):
        slot = lax.rem(g, nb)
        p0 = pr[32*p:32*p+16]; p1 = pr[32*p+16:32*p+32]
        pp = jnp.concatenate([jnp.concatenate([p0, zz], axis=1), jnp.concatenate([zz, p1], axis=1)], axis=0)
        vv = jnp.concatenate([vb[slot, 2*p], vb[slot, 2*p+1]], axis=1)
        o = lax.dot_general(pp, vv, (((1,), (1,)), ((), ())), preferred_element_type=F32)
        ev = []; od = []
        for j in (0, 1):
            oj = o[16*j:16*j+16]
            ev.append(jnp.sum(jnp.where(m_even[:8], oj[:8], 0.0), axis=0, keepdims=True))
            od.append(jnp.sum(jnp.where(m_even[:8], oj[8:], 0.0), axis=0, keepdims=True))
        return ev, od
    def attend(g, nxt):
        rows = pl.ds(pl.multiple_of(g*sb, sb), sb)
        qe = qe_ref[rows, :]
        qo = qo_ref[rows, :]
        sc = []
        for p in range(sb // 2):
            sc += scores(g, p, qe, qo)
        s = jnp.concatenate(sc, axis=0)
        e = jnp.exp(s - jnp.max(s, axis=-1, keepdims=True))
        pr = (e / jnp.sum(e, axis=-1, keepdims=True)).astype(BF)
        oe = []; oo = []
        for p in range(sb // 2):
            ev, od = combine(g, p, pr)
            oe += ev; oo += od
            if nxt is not None:
                insert(kb, kt_ref, nxt, p)
                insert(vb, vt_ref, nxt, p)
        ae_ref[rows, :] = jnp.concatenate(oe, axis=0)
        ao_ref[rows, :] = jnp.concatenate(oo, axis=0)

    cut = n // 2
    def finish(r0, nr):
        part = slice(r0, r0 + nr)
        y = h_ref[part].astype(F32)
        y = y + (jnp.dot(ae_ref[part].astype(BF), woe[...].reshape(dk, -1), preferred_element_type=F32)
                 + jnp.dot(ao_ref[part].astype(BF), woo[...].reshape(dk, -1), preferred_element_type=F32))
        y_ref[part] = y
        r = (y * lax.rsqrt(jnp.mean(y*y, axis=-1, keepdims=True) + EPS) * lnm_ref[...].astype(F32)[None, :]).astype(BF)
        r_ref[part] = r
        lg = lax.dot_general(wr_ref[...], r, (((1,), (1,)), ((), ())), preferred_element_type=F32)
        eid = lax.broadcasted_iota(jnp.int32, lg.shape, 0)
        ids = ids_ref[:, lo+r0:lo+r0+nr]
        hot = eid == ids[0:1]
        for j in range(1, ids.shape[0]):
            hot = hot | (eid == ids[j:j+1])
        lg = jnp.where(hot, lg, -jnp.inf)
        e = jnp.where(hot, jnp.exp(lg - jnp.max(lg, axis=0, keepdims=True)), 0.0)
        gt_ref[:, lo+r0:lo+r0+nr] = e / jnp.sum(e, axis=0, keepdims=True)
    if not first:
        gt_ref[:, :lo] = gp_ref[...]

    cin(0, 0).wait(); cin(0, 1).wait()
    for p in range(sb // 2):
        insert(kb, kt_ref, jnp.int32(0), p)
        insert(vb, vt_ref, jnp.int32(0), p)
    cout(0, 0).start(); cout(0, 1).start()
    for g in range(nb if first else 2, nb):
        cin(g, 0).start(); cin(g, 1).start()

    @pl.loop(0, steps - 1)
    def _(g):
        @pl.when((g >= lag) & (g - lag + nb < steps))
        def _():
            cout(g - lag, 0).wait(); cout(g - lag, 1).wait()
            cin(g - lag + nb, 0).start(); cin(g - lag + nb, 1).start()
        @pl.when(g == cut // sb)
        def _():
            for c in late:
                c.wait()
            finish(0, cut)
        cin(g + 1, 0).wait(); cin(g + 1, 1).wait()
        attend(g, g + 1)
        cout(g + 1, 0).start(); cout(g + 1, 1).start()
    attend(jnp.int32(steps - 1), None)

    finish(cut, n - cut)
    for j in range(nb):
        cout(steps - nb + j, 0).wait(); cout(steps - nb + j, 1).wait()

def attn_call(hidden, kc, vc, seq_lens, expert_ids, ln_attn, w_q, w_k, w_v, q_gain, k_gain, w_o, ln_moe, w_router, lo, n, prev=None, cfg=(8, 8, 3)):
    ntot, d = hidden.shape
    _, dk, t = kc.shape
    hd = q_gain.shape[0]
    nk = dk // hd
    sb, nb, lag = cfg
    ne = w_router.shape[1]
    first, last = lo == 0, lo + n == ntot
    vm = pl.BlockSpec(memory_space=pltpu.VMEM)
    an = pl.BlockSpec(memory_space=pltpu.HBM)
    args = [seq_lens, expert_ids.T, ln_moe, hidden, w_o.reshape(nk, 2, hd, d), w_router.T, kc, vc]
    specs = [an]*8
    alias = {}
    shape = jax.ShapeDtypeStruct
    outs = [shape(kc.shape, BF), shape(vc.shape, BF), shape((n, d), F32), shape((n, d), BF), shape((ne, lo + n), F32)]
    ospecs = [an, an, vm, vm, vm]
    dma = pltpu.SemaphoreType.DMA
    scratch = [pltpu.VMEM((nb, sb, dk, t), BF), pltpu.VMEM((nb, sb, dk, t), BF), pltpu.VMEM((nk, hd, d), BF), pltpu.VMEM((nk, hd, d), BF),
               pltpu.VMEM((ntot if first else n, d), BF), pltpu.VMEM((n, dk), F32), pltpu.VMEM((n, dk), F32),
               pltpu.SMEM(seq_lens.shape, jnp.int32), pltpu.VMEM(expert_ids.shape[::-1], jnp.int32), pltpu.VMEM(ln_moe.shape, BF), pltpu.VMEM(w_router.shape[::-1], BF),
               dma((2, nb)), dma((2, nb)), dma((7,))]
    if first:
        freq = np.power(np.float32(ROPE_BASE), -np.arange(0, hd, 2).astype(np.float32) / np.float32(hd)).astype(np.float32).reshape(-1, 1)
        args += [ln_attn, q_gain, k_gain, jnp.asarray(freq), w_q, w_k, w_v]
        specs += [an]*7
        scratch += [pltpu.VMEM((n, dk), F32), pltpu.VMEM((n, dk), F32), pltpu.VMEM((n//128, dk, 128), F32), pltpu.VMEM((n//128, dk, 128), F32),
                    pltpu.VMEM(w_q.shape, BF), pltpu.VMEM(w_k.shape, BF), pltpu.VMEM(w_v.shape, BF),
                    pltpu.VMEM(seq_lens.shape, jnp.int32), pltpu.VMEM(ln_attn.shape, BF), pltpu.VMEM(q_gain.shape, BF), pltpu.VMEM(k_gain.shape, BF), pltpu.VMEM(freq.shape, F32), dma((8,))]
        if not last:
            m = ntot - n
            outs += [shape((m, dk), F32), shape((m, dk), F32), shape((m//128, dk, 128), F32), shape((m//128, dk, 128), F32)]
            ospecs += [vm]*4
    else:
        args += list(prev)
        specs += [vm]*4 + [an, an, vm]
        alias = {12: 0, 13: 1}
    frac = n / ntot
    return pl.pallas_call(functools.partial(attn_body, cfg + (lo, n, first, last)), out_shape=outs, in_specs=specs, out_specs=ospecs,
        input_output_aliases=alias, scratch_shapes=scratch,
        compiler_params=pltpu.CompilerParams(vmem_limit_bytes=67043328), name="attn",
        cost_estimate=pl.CostEstimate(flops=int(40*10**9*frac), bytes_accessed=int(140*10**6*frac), transcendentals=0),
    )(*args)

def cache_views(c):
    n, t, nk, hd = c.shape
    return c.transpose(0, 2, 3, 1).reshape(n, nk*hd, t), lambda z: z.reshape(n, nk, hd, t).transpose(0, 3, 1, 2)


def moe_body(r_ref, gt_ref, y_hbm, wg_own, wu_own, wd_own, wg_par, wu_par, wd_par, out_ref,
             wg, wu, wd, xr, gts, y_ref, act, acc, rbuf, wsem, ysem, agsem_s, agsem_r, gsem_s, gsem_r, rssem_s, rssem_r):
    me = lax.axis_index('ep')
    core = me % 2
    xpos = (me // 2) % 2
    ypos = me // 4
    OWN, X, Y, D = 0, 1, 2, 3
    peers = [None, ypos*4 + (1-xpos)*2 + core, (1-ypos)*4 + xpos*2 + core, (1-ypos)*4 + (1-xpos)*2 + core]
    n_loc = wg_own.shape[0]
    n_exp = 2*n_loc
    hr, hc = acc.shape[3], acc.shape[4]
    ff = wg.shape[2]

    barrier = pltpu.get_barrier_semaphore()
    for p in peers[1:]:
        pl.semaphore_signal(barrier, inc=1, device_id={"ep": p}, device_id_type=pl.DeviceIdType.MESH)

    def wcopy(e, own):
        src = (wg_own, wu_own, wd_own) if own else (wg_par, wu_par, wd_par)
        s = lax.rem(e, n_loc)
        return [pltpu.make_async_copy(a.at[s], b.at[e], wsem.at[i, e]) for i, (a, b) in enumerate(zip(src, (wg, wu, wd)))]
    for c in wcopy(jnp.int32(0), True):
        c.start()
    ahead = 2
    for e in range(1, ahead):
        for c in wcopy(jnp.int32(e), True):
            c.start()
    ycopy = pltpu.make_async_copy(y_hbm, y_ref, ysem.at[0])
    ycopy.start()
    pl.semaphore_wait(barrier, 3)

    def remote(src, dst, ss, rs, p):
        return pltpu.make_async_remote_copy(src_ref=src, dst_ref=dst, send_sem=ss, recv_sem=rs,
                                            device_id={"ep": p}, device_id_type=pl.DeviceIdType.MESH)
    ag = {}
    gc = {}
    for b in (D, X, Y):
        rows8 = pl.ds(pl.multiple_of((peers[b] // 2) * n_exp, n_exp), n_exp)
        gc[b] = remote(gt_ref.at[rows8], gts.at[b-1], gsem_s.at[b-1], gsem_r.at[b-1], peers[b])
        gc[b].start()
    for b, h in ((X, 1), (Y, 0), (X, 0), (Y, 1)):
        part = pl.ds(h*hr, hr)
        ag[b, h] = remote(r_ref.at[part], xr.at[b-1, part], agsem_s.at[b-1, h], agsem_r.at[b-1, h], peers[b])
        ag[b, h].start()
    h0, h1 = pl.ds(0, hr), pl.ds(hr, hr)
    relay = [remote(xr.at[Y-1, h0], xr.at[D-1, h0], agsem_s.at[2, 0], agsem_r.at[2, 0], peers[X]),
             remote(xr.at[X-1, h1], xr.at[D-1, h1], agsem_s.at[2, 1], agsem_r.at[2, 1], peers[Y])]

    def gates(b):
        if b == OWN:
            return gt_ref[pl.ds(pl.multiple_of((me // 2) * n_exp, n_exp), n_exp), :].T
        return gts[b-1].T

    def compute(load, g8, blocks, first=False):
        m = len(blocks) * hr
        lane8 = lax.broadcasted_iota(jnp.int32, (m, n_exp), 1)
        for b, h in blocks:
            acc[b, h] = jnp.zeros(acc.shape[2:], F32)
        def step(e, carry):
            if first:
                for c in wcopy(e, True):
                    c.wait()
                @pl.when(e + ahead < n_loc)
                def _():
                    for c in wcopy(e + ahead, True):
                        c.start()
                @pl.when((e + ahead >= n_loc) & (e + ahead < n_exp))
                def _():
                    for c in wcopy(e + ahead, False):
                        c.start()
            gcol = jnp.sum(jnp.where(lane8 == lax.rem(core * n_loc + e, n_exp), g8, 0.0), axis=1, keepdims=True)
            x = load()
            for q in range(2):
                cols = slice(q*ff//2, (q+1)*ff//2)
                g = jnp.dot(x, wg[e, :, cols], preferred_element_type=F32)
                u = jnp.dot(x, wu[e, :, cols], preferred_element_type=F32)
                act[:m, cols] = (jax.nn.silu(g) * u).astype(BF)
            a = act[:m]
            for q in range(4):
                w = hc // 2
                s = (q % 2) * w
                f = jnp.dot(a, wd[e, :, q*w:(q+1)*w], preferred_element_type=F32).astype(BF).astype(F32) * gcol
                for i, (b, h) in enumerate(blocks):
                    acc[b, h, q//2, :, s:s+w] = acc[b, h, q//2, :, s:s+w] + f[i*hr:(i+1)*hr]
            return carry
        lax.fori_loop(0, n_exp, step, 0, unroll=1 if first else 2)

    def rs(i, h, src, p):
        return remote(src, rbuf.at[i, h], rssem_s.at[i, h], rssem_r.at[i, h], p)
    sent = {}
    def send(i, h, src, b):
        sent[i, h] = rs(i, h, src, peers[b])
        sent[i, h].start()

    def rows(h):
        return slice(h*hr, (h+1)*hr)
    def diagonal(h):
        relay[h].wait_recv()
        compute(lambda: xr[D-1, rows(h)], gates(D)[rows(h)], ((D, h),))
        send(0, h, acc.at[D, h, 0], X)
        send(1, h, acc.at[D, h, 1], Y)
    def neighbours(h):
        compute(lambda: jnp.concatenate([xr[X-1, rows(1-h)], xr[Y-1, rows(h)]], axis=0),
                jnp.concatenate([gates(X)[rows(1-h)], gates(Y)[rows(h)]], axis=0), ((X, 1-h), (Y, h)))
        send(2, 1-h, acc.at[X, 1-h, 0], X)
        send(3, h, acc.at[Y, h, 1], Y)
    def own(h, first):
        compute(lambda: r_ref[rows(h)], gates(OWN)[rows(h)], ((OWN, h),), first)
    def pass_on(h):
        sent[1, h].wait_recv()
        acc[X, h, 1] = acc[X, h, 1] + rbuf[1, h]
        send(4, h, acc.at[X, h, 1], X)
        sent[0, h].wait_recv()
        acc[Y, h, 0] = acc[Y, h, 0] + rbuf[0, h]
        send(5, h, acc.at[Y, h, 0], Y)
    own(0, True)
    ag[Y, 0].wait_recv()
    relay[0].start()
    ag[X, 1].wait_recv()
    relay[1].start()
    gc[X].wait_recv(); gc[Y].wait_recv()
    neighbours(0)
    ag[X, 0].wait_recv(); ag[Y, 1].wait_recv()
    neighbours(1)
    gc[D].wait_recv()
    diagonal(0)
    diagonal(1)
    own(1, False)
    pass_on(0)
    pass_on(1)
    ycopy.wait()
    for h in (0, 1):
        sent[2, h].wait_recv()
        sent[3, h].wait_recv()
        acc[OWN, h, 0] = y_ref[rows(h), :hc] + (acc[OWN, h, 0] + rbuf[2, h])
        acc[OWN, h, 1] = y_ref[rows(h), hc:] + (acc[OWN, h, 1] + rbuf[3, h])
        sent[5, h].wait_recv()
        out_ref[rows(h), :hc] = (acc[OWN, h, 0] + rbuf[5, h]).astype(out_ref.dtype)
        sent[4, h].wait_recv()
        out_ref[rows(h), hc:] = (acc[OWN, h, 1] + rbuf[4, h]).astype(out_ref.dtype)
    for c in (*gc.values(), *ag.values(), *relay, *sent.values()):
        c.wait_send()

def moe_call(r, gt, y, w_gate, w_up, w_down, wg_p, wu_p, wd_p):
    n, d = r.shape
    nl, _, ff = w_gate.shape
    vm = pl.BlockSpec(memory_space=pltpu.VMEM)
    an = pl.BlockSpec(memory_space=pl.ANY)
    dma = pltpu.SemaphoreType.DMA
    return pl.pallas_call(moe_body,
        out_shape=jax.ShapeDtypeStruct((n, d), BF),
        in_specs=[vm, vm] + [an]*7, out_specs=vm,
        scratch_shapes=[pltpu.VMEM((2*nl, d, ff), BF), pltpu.VMEM((2*nl, d, ff), BF), pltpu.VMEM((2*nl, ff, d), BF),
            pltpu.VMEM((3, n, d), BF), pltpu.VMEM((3, 2*nl, n), F32), pltpu.VMEM((n, d), F32), pltpu.VMEM((n, ff), BF),
            pltpu.VMEM((4, 2, 2, n//2, d//2), F32), pltpu.VMEM((6, 2, n//2, d//2), F32),
            dma((3, 2*nl)), dma((1,)), dma((3, 2)), dma((3, 2)), dma((3,)), dma((3,)), dma((6, 2)), dma((6, 2))],
        compiler_params=pltpu.CompilerParams(vmem_limit_bytes=67043328, collective_id=1, has_side_effects=True), name="moe",
        cost_estimate=pl.CostEstimate(flops=26*10**9, bytes_accessed=30*10**6, transcendentals=0),
    )(r, gt, y, w_gate, w_up, w_down, wg_p, wu_p, wd_p)


def solution(mesh):
    n_group = mesh.shape['ep']
    row_spec = P(('dp', 'ep'), None)
    cache_spec = P(('dp', 'ep'), None, None, None)
    len_spec = P(('dp', 'ep'))
    rep_vec = P(None)
    rep_mat = P(None, None)
    exp_spec = P('ep', None, None)
    swap = [(i, i + 1 - 2 * (i % 2)) for i in range(n_group)]

    def local_step(hidden, k_cache, v_cache, seq_lens, expert_ids, ln_attn, w_q, w_k, w_v, q_gain, k_gain, w_o, ln_moe, w_router, w_gate, w_up, w_down):
        wg_p = lax.ppermute(w_gate, 'ep', swap)
        wu_p = lax.ppermute(w_up, 'ep', swap)
        wd_p = lax.ppermute(w_down, 'ep', swap)
        kc, back = cache_views(k_cache)
        vc, _ = cache_views(v_cache)
        ko, vo, y, r, gt = attn_call(hidden, kc, vc, seq_lens, expert_ids, ln_attn, w_q, w_k, w_v, q_gain, k_gain, w_o, ln_moe, w_router, 0, hidden.shape[0])
        out = moe_call(r, gt, y, w_gate, w_up, w_down, wg_p, wu_p, wd_p)
        return out, back(ko), back(vo)

    return jax.shard_map(local_step, mesh=mesh, in_specs=(row_spec, cache_spec, cache_spec, len_spec, row_spec, rep_vec, rep_mat, rep_mat, rep_mat, rep_vec, rep_vec, rep_mat, rep_vec, rep_mat, exp_spec, exp_spec, exp_spec), out_specs=(row_spec, cache_spec, cache_spec), check_vma=False)
```

```python
import functools
import numpy as np
import jax, jax.numpy as jnp
from jax import lax
from jax.experimental import pallas as pl
from jax.experimental.pallas import tpu as pltpu
from jax.sharding import PartitionSpec as P
EPS=1e-6; ROPE_BASE=1e6
F32=jnp.float32; BF=jnp.bfloat16

def attn_body(cfg, lens_hbm, ids_hbm, lnm_hbm, h_hbm, wo_hbm, wr_hbm, k_hbm, v_hbm, *refs):
    sb, nb, lag, lo, n, first, last = cfg
    n_kv, hd, dk = 8, 64, 512
    if first:
        lna_hbm, qg_hbm, kg_hbm, freq_hbm, wq_hbm, wk_hbm, wv_hbm = refs[:7]
        refs = refs[7:]
    else:
        qe_ref, qo_ref, kt_ref, vt_ref, _, _, gp_ref = refs[:7]
        refs = refs[7:]
    ko_hbm, vo_hbm, y_ref, r_ref, gt_ref = refs[:5]
    refs = refs[5:]
    if first and not last:
        qeb_ref, qob_ref, ktb_ref, vtb_ref = refs[:4]
        refs = refs[4:]
    kb, vb, woe, woo, h_ref, ae_ref, ao_ref, lens_s, ids_ref, lnm_ref, wr_ref, isem, osem, wsem = refs[:14]
    if first:
        qe_ref, qo_ref, kt_ref, vt_ref, wq, wk, wv, lens_ref, lna_ref, qg_ref, kg_ref, freq_ref, qsem = refs[14:]
    steps = n // sb
    per = 128 // sb
    def cin(g, which):
        s = lax.rem(g, nb)
        r, b = ((k_hbm, kb), (v_hbm, vb))[which]
        return pltpu.make_async_copy(r.at[pl.ds(lo + g*sb, sb)], b.at[s], isem.at[which, s])
    def cout(g, which):
        s = lax.rem(g, nb)
        r, b = ((ko_hbm, kb), (vo_hbm, vb))[which]
        return pltpu.make_async_copy(b.at[s], r.at[pl.ds(lo + g*sb, sb)], osem.at[which, s])
    late = [pltpu.make_async_copy(a, b, wsem.at[i]) for i, (a, b) in enumerate(((wo_hbm.at[:, 0], woe), (wo_hbm.at[:, 1], woo), (ids_hbm, ids_ref), (lnm_hbm, lnm_ref), (wr_hbm, wr_ref)))]
    early = [pltpu.make_async_copy(h_hbm if first else h_hbm.at[pl.ds(lo, n)], h_ref, wsem.at[5]), pltpu.make_async_copy(lens_hbm, lens_s, wsem.at[6])]
    if first:
        early += [pltpu.make_async_copy(a, b, qsem.at[i]) for i, (a, b) in enumerate(((lens_hbm, lens_ref), (lna_hbm, lna_ref), (qg_hbm, qg_ref), (kg_hbm, kg_ref), (freq_hbm, freq_ref), (wq_hbm, wq), (wk_hbm, wk), (wv_hbm, wv)))]
    for c in early:
        c.start()
    if first:
        cin(0, 0).start(); cin(0, 1).start()
        for c in early:
            c.wait()
    for g in range(*((1, nb) if first else (0, 2))):
        cin(g, 0).start(); cin(g, 1).start()
    for c in late:
        c.start()
    if first:
        na = h_ref.shape[0]
        h = h_ref[...].astype(F32)
        x = (h * lax.rsqrt(jnp.mean(h*h, axis=-1, keepdims=True) + EPS) * lna_ref[...].astype(F32)[None, :]).astype(BF)
        ang = freq_ref[...] * lens_ref[...].astype(F32)[None, :]
        cos_v = jnp.cos(ang)[None]; sin_v = jnp.sin(ang)[None]
        half = hd // 2
        eye = lax.broadcasted_iota(jnp.int32, (hd, hd), 0) == lax.broadcasted_iota(jnp.int32, (hd, hd), 1)
        def norm_rope(w_ref, g_ref):
            gain = jnp.sum(jnp.where(eye, g_ref[...].astype(F32)[None, :], 0.0), axis=1, keepdims=True)
            p = jnp.dot(x, w_ref[...], preferred_element_type=F32)
            p = p.T.reshape(-1, hd, na)
            p = p * lax.rsqrt(jnp.mean(p*p, axis=1, keepdims=True) + EPS) * gain[None]
            lo_, hi = p[:, :half], p[:, half:]
            return jnp.concatenate([lo_*cos_v - hi*sin_v, hi*cos_v + lo_*sin_v], axis=1)
        q = norm_rope(wq, qg_ref)
        q = q.reshape(n_kv, 2, hd, na)
        qe = q[:, 0].reshape(dk, na).T
        qo = q[:, 1].reshape(dk, na).T
        qe_ref[...] = qe[:n]
        qo_ref[...] = qo[:n]
        k = norm_rope(wk, kg_ref).reshape(dk, na).astype(BF).astype(F32)
        v = jnp.dot(x, wv[...], preferred_element_type=F32).T.astype(BF).astype(F32)
        for c in range(n // 128):
            kt_ref[c] = k[:, 128*c:128*c+128]
            vt_ref[c] = v[:, 128*c:128*c+128]
        if not last:
            qeb_ref[...] = qe[n:]
            qob_ref[...] = qo[n:]
            for c in range((na - n) // 128):
                ktb_ref[c] = k[:, n+128*c:n+128*c+128]
                vtb_ref[c] = v[:, n+128*c:n+128*c+128]
    else:
        for c in early:
            c.wait()

    lane = lax.broadcasted_iota(jnp.int32, (1, 128), 1)
    row = lax.broadcasted_iota(jnp.int32, (16, dk), 0)
    col = lax.broadcasted_iota(jnp.int32, (16, dk), 1) // hd
    m_even = row == col
    m_odd = row == col + n_kv

    zz = jnp.zeros((16, 128), BF)
    def fresh(t_ref, g, i):
        ln = lens_s[lo + g*sb + i]
        col = pltpu.roll(t_ref[g // per], lax.rem(ln - (lax.rem(g, per) * sb + i) + 128, 128), 1).astype(BF)
        return lane == ln, col
    def insert(buf, t_ref, g, p):
        slot = lax.rem(g, nb)
        for i in (2*p, 2*p+1):
            hit, col = fresh(t_ref, g, i)
            buf[slot, i] = jnp.where(hit, col, buf[slot, i])
    def scores(g, p, qe, qo):
        slot = lax.rem(g, nb)
        qs = [jnp.where(m_even, qe[i:i+1], jnp.where(m_odd, qo[i:i+1], 0.0)).astype(BF) for i in (2*p, 2*p+1)]
        ks = jnp.concatenate([kb[slot, 2*p], kb[slot, 2*p+1]], axis=1)
        s = jnp.dot(jnp.concatenate(qs, axis=0), ks, preferred_element_type=F32)
        return [jnp.where(lane <= lens_s[lo + g*sb + 2*p + j], s[16*j:16*j+16, 128*j:128*j+128] * (hd ** -0.5), -1e30) for j in (0, 1)]
    def combine(g, p, pr):
        slot = lax.rem(g, nb)
        p0 = pr[32*p:32*p+16]; p1 = pr[32*p+16:32*p+32]
        pp = jnp.concatenate([jnp.concatenate([p0, zz], axis=1), jnp.concatenate([zz, p1], axis=1)], axis=0)
        vv = jnp.concatenate([vb[slot, 2*p], vb[slot, 2*p+1]], axis=1)
        o = lax.dot_general(pp, vv, (((1,), (1,)), ((), ())), preferred_element_type=F32)
        ev = []; od = []
        for j in (0, 1):
            oj = o[16*j:16*j+16]
            ev.append(jnp.sum(jnp.where(m_even[:8], oj[:8], 0.0), axis=0, keepdims=True))
            od.append(jnp.sum(jnp.where(m_even[:8], oj[8:], 0.0), axis=0, keepdims=True))
        return ev, od
    def attend(g, nxt):
        rows = pl.ds(pl.multiple_of(g*sb, sb), sb)
        qe = qe_ref[rows, :]
        qo = qo_ref[rows, :]
        sc = []
        for p in range(sb // 2):
            sc += scores(g, p, qe, qo)
        s = jnp.concatenate(sc, axis=0)
        e = jnp.exp(s - jnp.max(s, axis=-1, keepdims=True))
        pr = (e / jnp.sum(e, axis=-1, keepdims=True)).astype(BF)
        oe = []; oo = []
        for p in range(sb // 2):
            ev, od = combine(g, p, pr)
            oe += ev; oo += od
            if nxt is not None:
                insert(kb, kt_ref, nxt, p)
                insert(vb, vt_ref, nxt, p)
        ae_ref[rows, :] = jnp.concatenate(oe, axis=0)
        ao_ref[rows, :] = jnp.concatenate(oo, axis=0)

    cut = n // 2
    def finish(r0, nr):
        part = slice(r0, r0 + nr)
        y = h_ref[part].astype(F32)
        y = y + (jnp.dot(ae_ref[part].astype(BF), woe[...].reshape(dk, -1), preferred_element_type=F32)
                 + jnp.dot(ao_ref[part].astype(BF), woo[...].reshape(dk, -1), preferred_element_type=F32))
        y_ref[part] = y
        r = (y * lax.rsqrt(jnp.mean(y*y, axis=-1, keepdims=True) + EPS) * lnm_ref[...].astype(F32)[None, :]).astype(BF)
        r_ref[part] = r
        lg = lax.dot_general(wr_ref[...], r, (((1,), (1,)), ((), ())), preferred_element_type=F32)
        eid = lax.broadcasted_iota(jnp.int32, lg.shape, 0)
        ids = ids_ref[:, lo+r0:lo+r0+nr]
        hot = eid == ids[0:1]
        for j in range(1, ids.shape[0]):
            hot = hot | (eid == ids[j:j+1])
        lg = jnp.where(hot, lg, -jnp.inf)
        e = jnp.where(hot, jnp.exp(lg - jnp.max(lg, axis=0, keepdims=True)), 0.0)
        gt_ref[:, lo+r0:lo+r0+nr] = e / jnp.sum(e, axis=0, keepdims=True)
    if not first:
        gt_ref[:, :lo] = gp_ref[...]

    cin(0, 0).wait(); cin(0, 1).wait()
    for p in range(sb // 2):
        insert(kb, kt_ref, jnp.int32(0), p)
        insert(vb, vt_ref, jnp.int32(0), p)
    cout(0, 0).start(); cout(0, 1).start()
    for g in range(nb if first else 2, nb):
        cin(g, 0).start(); cin(g, 1).start()

    @pl.loop(0, steps - 1)
    def _(g):
        @pl.when((g >= lag) & (g - lag + nb < steps))
        def _():
            cout(g - lag, 0).wait(); cout(g - lag, 1).wait()
            cin(g - lag + nb, 0).start(); cin(g - lag + nb, 1).start()
        @pl.when(g == cut // sb)
        def _():
            for c in late:
                c.wait()
            finish(0, cut)
        cin(g + 1, 0).wait(); cin(g + 1, 1).wait()
        attend(g, g + 1)
        cout(g + 1, 0).start(); cout(g + 1, 1).start()
    attend(jnp.int32(steps - 1), None)

    finish(cut, n - cut)
    for j in range(nb):
        cout(steps - nb + j, 0).wait(); cout(steps - nb + j, 1).wait()

def attn_call(hidden, kc, vc, seq_lens, expert_ids, ln_attn, w_q, w_k, w_v, q_gain, k_gain, w_o, ln_moe, w_router, lo, n, prev=None, cfg=(8, 8, 2)):
    ntot, d = hidden.shape
    _, dk, t = kc.shape
    hd = q_gain.shape[0]
    nk = dk // hd
    sb, nb, lag = cfg
    ne = w_router.shape[1]
    first, last = lo == 0, lo + n == ntot
    vm = pl.BlockSpec(memory_space=pltpu.VMEM)
    an = pl.BlockSpec(memory_space=pltpu.HBM)
    args = [seq_lens, expert_ids.T, ln_moe, hidden, w_o.reshape(nk, 2, hd, d), w_router.T, kc, vc]
    specs = [an]*8
    alias = {}
    shape = jax.ShapeDtypeStruct
    outs = [shape(kc.shape, BF), shape(vc.shape, BF), shape((n, d), F32), shape((n, d), BF), shape((ne, lo + n), F32)]
    ospecs = [an, an, vm, vm, vm]
    dma = pltpu.SemaphoreType.DMA
    scratch = [pltpu.VMEM((nb, sb, dk, t), BF), pltpu.VMEM((nb, sb, dk, t), BF), pltpu.VMEM((nk, hd, d), BF), pltpu.VMEM((nk, hd, d), BF),
               pltpu.VMEM((ntot if first else n, d), BF), pltpu.VMEM((n, dk), F32), pltpu.VMEM((n, dk), F32),
               pltpu.SMEM(seq_lens.shape, jnp.int32), pltpu.VMEM(expert_ids.shape[::-1], jnp.int32), pltpu.VMEM(ln_moe.shape, BF), pltpu.VMEM(w_router.shape[::-1], BF),
               dma((2, nb)), dma((2, nb)), dma((7,))]
    if first:
        freq = np.power(np.float32(ROPE_BASE), -np.arange(0, hd, 2).astype(np.float32) / np.float32(hd)).astype(np.float32).reshape(-1, 1)
        args += [ln_attn, q_gain, k_gain, jnp.asarray(freq), w_q, w_k, w_v]
        specs += [an]*7
        scratch += [pltpu.VMEM((n, dk), F32), pltpu.VMEM((n, dk), F32), pltpu.VMEM((n//128, dk, 128), F32), pltpu.VMEM((n//128, dk, 128), F32),
                    pltpu.VMEM(w_q.shape, BF), pltpu.VMEM(w_k.shape, BF), pltpu.VMEM(w_v.shape, BF),
                    pltpu.VMEM(seq_lens.shape, jnp.int32), pltpu.VMEM(ln_attn.shape, BF), pltpu.VMEM(q_gain.shape, BF), pltpu.VMEM(k_gain.shape, BF), pltpu.VMEM(freq.shape, F32), dma((8,))]
        if not last:
            m = ntot - n
            outs += [shape((m, dk), F32), shape((m, dk), F32), shape((m//128, dk, 128), F32), shape((m//128, dk, 128), F32)]
            ospecs += [vm]*4
    else:
        args += list(prev)
        specs += [vm]*4 + [an, an, vm]
        alias = {12: 0, 13: 1}
    frac = n / ntot
    return pl.pallas_call(functools.partial(attn_body, cfg + (lo, n, first, last)), out_shape=outs, in_specs=specs, out_specs=ospecs,
        input_output_aliases=alias, scratch_shapes=scratch,
        compiler_params=pltpu.CompilerParams(vmem_limit_bytes=67043328), name="attn",
        cost_estimate=pl.CostEstimate(flops=int(40*10**9*frac), bytes_accessed=int(140*10**6*frac), transcendentals=0),
    )(*args)

def cache_views(c):
    n, t, nk, hd = c.shape
    return c.transpose(0, 2, 3, 1).reshape(n, nk*hd, t), lambda z: z.reshape(n, nk, hd, t).transpose(0, 3, 1, 2)


def moe_body(r_hbm, gt_hbm, y_hbm, wg_own, wu_own, wd_own, wg_par, wu_par, wd_par, out_ref,
             wg, wu, wd, r_ref, gt_ref, xr, gts, y_ref, act, acc, rbuf, wsem, ysem, agsem_s, agsem_r, gsem_s, gsem_r, rssem_s, rssem_r):
    me = lax.axis_index('ep')
    core = me % 2
    xpos = (me // 2) % 2
    ypos = me // 4
    OWN, X, Y, D = 0, 1, 2, 3
    peers = [None, ypos*4 + (1-xpos)*2 + core, (1-ypos)*4 + xpos*2 + core, (1-ypos)*4 + (1-xpos)*2 + core]
    n_loc = wg_own.shape[0]
    n_exp = 2*n_loc
    hr, hc = acc.shape[3], acc.shape[4]
    ff = wg.shape[2]

    mine = [pltpu.make_async_copy(a, b, ysem.at[i]) for i, (a, b) in enumerate(((r_hbm, r_ref), (gt_hbm, gt_ref)))]
    for c in mine:
        c.start()
    barrier = pltpu.get_barrier_semaphore()
    for p in peers[1:]:
        pl.semaphore_signal(barrier, inc=1, device_id={"ep": p}, device_id_type=pl.DeviceIdType.MESH)

    def wcopy(e, own):
        src = (wg_own, wu_own, wd_own) if own else (wg_par, wu_par, wd_par)
        s = lax.rem(e, n_loc)
        return [pltpu.make_async_copy(a.at[s], b.at[e], wsem.at[i, e]) for i, (a, b) in enumerate(zip(src, (wg, wu, wd)))]
    for c in wcopy(jnp.int32(0), True):
        c.start()
    ahead = 2
    for e in range(1, ahead):
        for c in wcopy(jnp.int32(e), True):
            c.start()
    ycopy = pltpu.make_async_copy(y_hbm, y_ref, ysem.at[2])
    ycopy.start()
    for c in mine:
        c.wait()
    pl.semaphore_wait(barrier, 3)

    def remote(src, dst, ss, rs, p):
        return pltpu.make_async_remote_copy(src_ref=src, dst_ref=dst, send_sem=ss, recv_sem=rs,
                                            device_id={"ep": p}, device_id_type=pl.DeviceIdType.MESH)
    ag = {}
    gc = {}
    for b in (D, X, Y):
        rows8 = pl.ds(pl.multiple_of((peers[b] // 2) * n_exp, n_exp), n_exp)
        gc[b] = remote(gt_ref.at[rows8], gts.at[b-1], gsem_s.at[b-1], gsem_r.at[b-1], peers[b])
        gc[b].start()
    for b, h in ((X, 1), (Y, 0), (X, 0), (Y, 1)):
        part = pl.ds(h*hr, hr)
        ag[b, h] = remote(r_ref.at[part], xr.at[b-1, part], agsem_s.at[b-1, h], agsem_r.at[b-1, h], peers[b])
        ag[b, h].start()
    h0, h1 = pl.ds(0, hr), pl.ds(hr, hr)
    relay = [remote(xr.at[Y-1, h0], xr.at[D-1, h0], agsem_s.at[2, 0], agsem_r.at[2, 0], peers[X]),
             remote(xr.at[X-1, h1], xr.at[D-1, h1], agsem_s.at[2, 1], agsem_r.at[2, 1], peers[Y])]

    def gates(b):
        if b == OWN:
            return gt_ref[pl.ds(pl.multiple_of((me // 2) * n_exp, n_exp), n_exp), :].T
        return gts[b-1].T

    def compute(load, g8, blocks, first=False):
        m = len(blocks) * hr
        lane8 = lax.broadcasted_iota(jnp.int32, (m, n_exp), 1)
        for b, h in blocks:
            acc[b, h] = jnp.zeros(acc.shape[2:], F32)
        def step(e, carry):
            if first:
                for c in wcopy(e, True):
                    c.wait()
                @pl.when(e + ahead < n_loc)
                def _():
                    for c in wcopy(e + ahead, True):
                        c.start()
                @pl.when((e + ahead >= n_loc) & (e + ahead < n_exp))
                def _():
                    for c in wcopy(e + ahead, False):
                        c.start()
            gcol = jnp.sum(jnp.where(lane8 == lax.rem(core * n_loc + e, n_exp), g8, 0.0), axis=1, keepdims=True)
            x = load()
            for q in range(2):
                cols = slice(q*ff//2, (q+1)*ff//2)
                g = jnp.dot(x, wg[e, :, cols], preferred_element_type=F32)
                u = jnp.dot(x, wu[e, :, cols], preferred_element_type=F32)
                act[:m, cols] = (jax.nn.silu(g) * u).astype(BF)
            a = act[:m]
            for q in range(4):
                w = hc // 2
                s = (q % 2) * w
                f = jnp.dot(a, wd[e, :, q*w:(q+1)*w], preferred_element_type=F32).astype(BF).astype(F32) * gcol
                for i, (b, h) in enumerate(blocks):
                    acc[b, h, q//2, :, s:s+w] = acc[b, h, q//2, :, s:s+w] + f[i*hr:(i+1)*hr]
            return carry
        lax.fori_loop(0, n_exp, step, 0, unroll=1 if first else 2)

    def rs(i, h, src, p):
        return remote(src, rbuf.at[i, h], rssem_s.at[i, h], rssem_r.at[i, h], p)
    sent = {}
    def send(i, h, src, b):
        sent[i, h] = rs(i, h, src, peers[b])
        sent[i, h].start()

    def rows(h):
        return slice(h*hr, (h+1)*hr)
    def diagonal(h):
        relay[h].wait_recv()
        compute(lambda: xr[D-1, rows(h)], gates(D)[rows(h)], ((D, h),))
        send(0, h, acc.at[D, h, 0], X)
        send(1, h, acc.at[D, h, 1], Y)
    def neighbours(h):
        compute(lambda: jnp.concatenate([xr[X-1, rows(1-h)], xr[Y-1, rows(h)]], axis=0),
                jnp.concatenate([gates(X)[rows(1-h)], gates(Y)[rows(h)]], axis=0), ((X, 1-h), (Y, h)))
        send(2, 1-h, acc.at[X, 1-h, 0], X)
        send(3, h, acc.at[Y, h, 1], Y)
    def own(h, first):
        compute(lambda: r_ref[rows(h)], gates(OWN)[rows(h)], ((OWN, h),), first)
    def pass_on(h):
        sent[1, h].wait_recv()
        acc[X, h, 1] = acc[X, h, 1] + rbuf[1, h]
        send(4, h, acc.at[X, h, 1], X)
        sent[0, h].wait_recv()
        acc[Y, h, 0] = acc[Y, h, 0] + rbuf[0, h]
        send(5, h, acc.at[Y, h, 0], Y)
    own(0, True)
    ag[Y, 0].wait_recv()
    relay[0].start()
    ag[X, 1].wait_recv()
    relay[1].start()
    gc[X].wait_recv(); gc[Y].wait_recv()
    neighbours(0)
    ag[X, 0].wait_recv(); ag[Y, 1].wait_recv()
    neighbours(1)
    gc[D].wait_recv()
    diagonal(0)
    diagonal(1)
    own(1, False)
    pass_on(0)
    pass_on(1)
    ycopy.wait()
    for h in (0, 1):
        sent[2, h].wait_recv()
        sent[3, h].wait_recv()
        acc[OWN, h, 0] = y_ref[rows(h), :hc] + (acc[OWN, h, 0] + rbuf[2, h])
        acc[OWN, h, 1] = y_ref[rows(h), hc:] + (acc[OWN, h, 1] + rbuf[3, h])
        sent[5, h].wait_recv()
        out_ref[rows(h), :hc] = (acc[OWN, h, 0] + rbuf[5, h]).astype(out_ref.dtype)
        sent[4, h].wait_recv()
        out_ref[rows(h), hc:] = (acc[OWN, h, 1] + rbuf[4, h]).astype(out_ref.dtype)
    for c in (*gc.values(), *ag.values(), *relay, *sent.values()):
        c.wait_send()

def moe_call(r, gt, y, w_gate, w_up, w_down, wg_p, wu_p, wd_p):
    n, d = r.shape
    nl, _, ff = w_gate.shape
    vm = pl.BlockSpec(memory_space=pltpu.VMEM)
    an = pl.BlockSpec(memory_space=pl.ANY)
    dma = pltpu.SemaphoreType.DMA
    return pl.pallas_call(moe_body,
        out_shape=jax.ShapeDtypeStruct((n, d), BF),
        in_specs=[an]*9, out_specs=vm,
        scratch_shapes=[pltpu.VMEM((2*nl, d, ff), BF), pltpu.VMEM((2*nl, d, ff), BF), pltpu.VMEM((2*nl, ff, d), BF),
            pltpu.VMEM(r.shape, BF), pltpu.VMEM(gt.shape, F32), pltpu.VMEM((3, n, d), BF), pltpu.VMEM((3, 2*nl, n), F32), pltpu.VMEM((n, d), F32), pltpu.VMEM((n, ff), BF),
            pltpu.VMEM((4, 2, 2, n//2, d//2), F32), pltpu.VMEM((6, 2, n//2, d//2), F32),
            dma((3, 2*nl)), dma((3,)), dma((3, 2)), dma((3, 2)), dma((3,)), dma((3,)), dma((6, 2)), dma((6, 2))],
        compiler_params=pltpu.CompilerParams(vmem_limit_bytes=67043328, collective_id=1, has_side_effects=True), name="moe",
        cost_estimate=pl.CostEstimate(flops=26*10**9, bytes_accessed=30*10**6, transcendentals=0),
    )(r, gt, y, w_gate, w_up, w_down, wg_p, wu_p, wd_p)


def solution(mesh):
    n_group = mesh.shape['ep']
    row_spec = P(('dp', 'ep'), None)
    cache_spec = P(('dp', 'ep'), None, None, None)
    len_spec = P(('dp', 'ep'))
    rep_vec = P(None)
    rep_mat = P(None, None)
    exp_spec = P('ep', None, None)
    swap = [(i, i + 1 - 2 * (i % 2)) for i in range(n_group)]

    def local_step(hidden, k_cache, v_cache, seq_lens, expert_ids, ln_attn, w_q, w_k, w_v, q_gain, k_gain, w_o, ln_moe, w_router, w_gate, w_up, w_down):
        wg_p = lax.ppermute(w_gate, 'ep', swap)
        wu_p = lax.ppermute(w_up, 'ep', swap)
        wd_p = lax.ppermute(w_down, 'ep', swap)
        kc, back = cache_views(k_cache)
        vc, _ = cache_views(v_cache)
        ko, vo, y, r, gt = attn_call(hidden, kc, vc, seq_lens, expert_ids, ln_attn, w_q, w_k, w_v, q_gain, k_gain, w_o, ln_moe, w_router, 0, hidden.shape[0])
        out = moe_call(r, gt, y, w_gate, w_up, w_down, wg_p, wu_p, wd_p)
        return out, back(ko), back(vo)

    return jax.shard_map(local_step, mesh=mesh, in_specs=(row_spec, cache_spec, cache_spec, len_spec, row_spec, rep_vec, rep_mat, rep_mat, rep_mat, rep_vec, rep_vec, rep_mat, rep_vec, rep_mat, exp_spec, exp_spec, exp_spec), out_specs=(row_spec, cache_spec, cache_spec), check_vma=False)
```

```python
import functools
import numpy as np
import jax, jax.numpy as jnp
from jax import lax
from jax.experimental import pallas as pl
from jax.experimental.pallas import tpu as pltpu
from jax.sharding import PartitionSpec as P
EPS=1e-6; ROPE_BASE=1e6
F32=jnp.float32; BF=jnp.bfloat16

def attn_body(cfg, lens_hbm, ids_hbm, lnm_hbm, h_hbm, wo_hbm, wr_hbm, k_hbm, v_hbm, *refs):
    sb, nb, lag, lo, n, first, last = cfg
    n_kv, hd, dk = 8, 64, 512
    if first:
        lna_hbm, qg_hbm, kg_hbm, freq_hbm, wq_hbm, wk_hbm, wv_hbm = refs[:7]
        refs = refs[7:]
    else:
        qe_ref, qo_ref, kt_ref, vt_ref, _, _, gp_ref = refs[:7]
        refs = refs[7:]
    ko_hbm, vo_hbm, y_ref, r_ref, gt_ref = refs[:5]
    refs = refs[5:]
    if first and not last:
        qeb_ref, qob_ref, ktb_ref, vtb_ref = refs[:4]
        refs = refs[4:]
    kb, vb, woe, woo, h_ref, ae_ref, ao_ref, lens_s, ids_ref, lnm_ref, wr_ref, isem, osem, wsem = refs[:14]
    if first:
        qe_ref, qo_ref, kt_ref, vt_ref, wq, wk, wv, lens_ref, lna_ref, qg_ref, kg_ref, freq_ref, qsem = refs[14:]
    steps = n // sb
    per = 128 // sb
    def cin(g, which):
        s = lax.rem(g, nb)
        r, b = ((k_hbm, kb), (v_hbm, vb))[which]
        return pltpu.make_async_copy(r.at[pl.ds(lo + g*sb, sb)], b.at[s], isem.at[which, s])
    def cout(g, which):
        s = lax.rem(g, nb)
        r, b = ((ko_hbm, kb), (vo_hbm, vb))[which]
        return pltpu.make_async_copy(b.at[s], r.at[pl.ds(lo + g*sb, sb)], osem.at[which, s])
    late = [pltpu.make_async_copy(a, b, wsem.at[i]) for i, (a, b) in enumerate(((wo_hbm.at[:, 0], woe), (wo_hbm.at[:, 1], woo), (ids_hbm, ids_ref), (lnm_hbm, lnm_ref), (wr_hbm, wr_ref)))]
    early = [pltpu.make_async_copy(h_hbm if first else h_hbm.at[pl.ds(lo, n)], h_ref, wsem.at[5]), pltpu.make_async_copy(lens_hbm, lens_s, wsem.at[6])]
    if first:
        early += [pltpu.make_async_copy(a, b, qsem.at[i]) for i, (a, b) in enumerate(((lens_hbm, lens_ref), (lna_hbm, lna_ref), (qg_hbm, qg_ref), (kg_hbm, kg_ref), (freq_hbm, freq_ref), (wq_hbm, wq), (wk_hbm, wk), (wv_hbm, wv)))]
    for c in early:
        c.start()
    if first:
        cin(0, 0).start(); cin(0, 1).start()
        for c in early:
            c.wait()
    for g in range(*((1, nb) if first else (0, 2))):
        cin(g, 0).start(); cin(g, 1).start()
    for c in late:
        c.start()
    if first:
        na = h_ref.shape[0]
        h = h_ref[...].astype(F32)
        x = (h * lax.rsqrt(jnp.mean(h*h, axis=-1, keepdims=True) + EPS) * lna_ref[...].astype(F32)[None, :]).astype(BF)
        ang = freq_ref[...] * lens_ref[...].astype(F32)[None, :]
        cos_v = jnp.cos(ang)[None]; sin_v = jnp.sin(ang)[None]
        half = hd // 2
        eye = lax.broadcasted_iota(jnp.int32, (hd, hd), 0) == lax.broadcasted_iota(jnp.int32, (hd, hd), 1)
        def norm_rope(w_ref, g_ref):
            gain = jnp.sum(jnp.where(eye, g_ref[...].astype(F32)[None, :], 0.0), axis=1, keepdims=True)
            p = jnp.dot(x, w_ref[...], preferred_element_type=F32)
            p = p.T.reshape(-1, hd, na)
            p = p * lax.rsqrt(jnp.mean(p*p, axis=1, keepdims=True) + EPS) * gain[None]
            lo_, hi = p[:, :half], p[:, half:]
            return jnp.concatenate([lo_*cos_v - hi*sin_v, hi*cos_v + lo_*sin_v], axis=1)
        q = norm_rope(wq, qg_ref)
        q = q.reshape(n_kv, 2, hd, na)
        qe = q[:, 0].reshape(dk, na).T
        qo = q[:, 1].reshape(dk, na).T
        qe_ref[...] = qe[:n]
        qo_ref[...] = qo[:n]
        k = norm_rope(wk, kg_ref).reshape(dk, na).astype(BF).astype(F32)
        v = jnp.dot(x, wv[...], preferred_element_type=F32).T.astype(BF).astype(F32)
        for c in range(n // 128):
            kt_ref[c] = k[:, 128*c:128*c+128]
            vt_ref[c] = v[:, 128*c:128*c+128]
        if not last:
            qeb_ref[...] = qe[n:]
            qob_ref[...] = qo[n:]
            for c in range((na - n) // 128):
                ktb_ref[c] = k[:, n+128*c:n+128*c+128]
                vtb_ref[c] = v[:, n+128*c:n+128*c+128]
    else:
        for c in early:
            c.wait()

    lane = lax.broadcasted_iota(jnp.int32, (1, 128), 1)
    row = lax.broadcasted_iota(jnp.int32, (16, dk), 0)
    col = lax.broadcasted_iota(jnp.int32, (16, dk), 1) // hd
    m_even = row == col
    m_odd = row == col + n_kv

    zz = jnp.zeros((16, 128), BF)
    def fresh(t_ref, g, i):
        ln = lens_s[lo + g*sb + i]
        col = pltpu.roll(t_ref[g // per], lax.rem(ln - (lax.rem(g, per) * sb + i) + 128, 128), 1).astype(BF)
        return lane == ln, col
    def insert(buf, t_ref, g, p):
        slot = lax.rem(g, nb)
        for i in (2*p, 2*p+1):
            hit, col = fresh(t_ref, g, i)
            buf[slot, i] = jnp.where(hit, col, buf[slot, i])
    def scores(g, p, qe, qo):
        slot = lax.rem(g, nb)
        qs = [jnp.where(m_even, qe[i:i+1], jnp.where(m_odd, qo[i:i+1], 0.0)).astype(BF) for i in (2*p, 2*p+1)]
        ks = jnp.concatenate([kb[slot, 2*p], kb[slot, 2*p+1]], axis=1)
        s = jnp.dot(jnp.concatenate(qs, axis=0), ks, preferred_element_type=F32)
        return [jnp.where(lane <= lens_s[lo + g*sb + 2*p + j], s[16*j:16*j+16, 128*j:128*j+128] * (hd ** -0.5), -1e30) for j in (0, 1)]
    def combine(g, p, pr):
        slot = lax.rem(g, nb)
        p0 = pr[32*p:32*p+16]; p1 = pr[32*p+16:32*p+32]
        pp = jnp.concatenate([jnp.concatenate([p0, zz], axis=1), jnp.concatenate([zz, p1], axis=1)], axis=0)
        vv = jnp.concatenate([vb[slot, 2*p], vb[slot, 2*p+1]], axis=1)
        o = lax.dot_general(pp, vv, (((1,), (1,)), ((), ())), preferred_element_type=F32)
        ev = []; od = []
        for j in (0, 1):
            oj = o[16*j:16*j+16]
            ev.append(jnp.sum(jnp.where(m_even[:8], oj[:8], 0.0), axis=0, keepdims=True))
            od.append(jnp.sum(jnp.where(m_even[:8], oj[8:], 0.0), axis=0, keepdims=True))
        return ev, od
    def attend(g, nxt):
        rows = pl.ds(pl.multiple_of(g*sb, sb), sb)
        qe = qe_ref[rows, :]
        qo = qo_ref[rows, :]
        sc = []
        for p in range(sb // 2):
            sc += scores(g, p, qe, qo)
        s = jnp.concatenate(sc, axis=0)
        e = jnp.exp(s - jnp.max(s, axis=-1, keepdims=True))
        pr = (e / jnp.sum(e, axis=-1, keepdims=True)).astype(BF)
        oe = []; oo = []
        for p in range(sb // 2):
            ev, od = combine(g, p, pr)
            oe += ev; oo += od
            if nxt is not None:
                insert(kb, kt_ref, nxt, p)
                insert(vb, vt_ref, nxt, p)
        ae_ref[rows, :] = jnp.concatenate(oe, axis=0)
        ao_ref[rows, :] = jnp.concatenate(oo, axis=0)

    cut = n // 2
    def finish(r0, nr):
        part = slice(r0, r0 + nr)
        y = h_ref[part].astype(F32)
        y = y + (jnp.dot(ae_ref[part].astype(BF), woe[...].reshape(dk, -1), preferred_element_type=F32)
                 + jnp.dot(ao_ref[part].astype(BF), woo[...].reshape(dk, -1), preferred_element_type=F32))
        y_ref[part] = y
        r = (y * lax.rsqrt(jnp.mean(y*y, axis=-1, keepdims=True) + EPS) * lnm_ref[...].astype(F32)[None, :]).astype(BF)
        r_ref[part] = r
        lg = lax.dot_general(wr_ref[...], r, (((1,), (1,)), ((), ())), preferred_element_type=F32)
        eid = lax.broadcasted_iota(jnp.int32, lg.shape, 0)
        ids = ids_ref[:, lo+r0:lo+r0+nr]
        hot = eid == ids[0:1]
        for j in range(1, ids.shape[0]):
            hot = hot | (eid == ids[j:j+1])
        lg = jnp.where(hot, lg, -jnp.inf)
        e = jnp.where(hot, jnp.exp(lg - jnp.max(lg, axis=0, keepdims=True)), 0.0)
        gt_ref[:, lo+r0:lo+r0+nr] = e / jnp.sum(e, axis=0, keepdims=True)
    if not first:
        gt_ref[:, :lo] = gp_ref[...]

    cin(0, 0).wait(); cin(0, 1).wait()
    for p in range(sb // 2):
        insert(kb, kt_ref, jnp.int32(0), p)
        insert(vb, vt_ref, jnp.int32(0), p)
    cout(0, 0).start(); cout(0, 1).start()
    for g in range(nb if first else 2, nb):
        cin(g, 0).start(); cin(g, 1).start()

    @pl.loop(0, steps - 1)
    def _(g):
        @pl.when((g >= lag) & (g - lag + nb < steps))
        def _():
            cout(g - lag, 0).wait(); cout(g - lag, 1).wait()
            cin(g - lag + nb, 0).start(); cin(g - lag + nb, 1).start()
        @pl.when(g == cut // sb)
        def _():
            for c in late:
                c.wait()
            finish(0, cut)
        cin(g + 1, 0).wait(); cin(g + 1, 1).wait()
        attend(g, g + 1)
        cout(g + 1, 0).start(); cout(g + 1, 1).start()
    attend(jnp.int32(steps - 1), None)

    finish(cut, n - cut)
    for j in range(nb):
        cout(steps - nb + j, 0).wait(); cout(steps - nb + j, 1).wait()

def attn_call(hidden, kc, vc, seq_lens, expert_ids, ln_attn, w_q, w_k, w_v, q_gain, k_gain, w_o, ln_moe, w_router, lo, n, prev=None, cfg=(8, 8, 2)):
    ntot, d = hidden.shape
    _, dk, t = kc.shape
    hd = q_gain.shape[0]
    nk = dk // hd
    sb, nb, lag = cfg
    ne = w_router.shape[1]
    first, last = lo == 0, lo + n == ntot
    vm = pl.BlockSpec(memory_space=pltpu.VMEM)
    an = pl.BlockSpec(memory_space=pltpu.HBM)
    args = [seq_lens, expert_ids.T, ln_moe, hidden, w_o.reshape(nk, 2, hd, d), w_router.T, kc, vc]
    specs = [an]*8
    alias = {}
    shape = jax.ShapeDtypeStruct
    outs = [shape(kc.shape, BF), shape(vc.shape, BF), shape((n, d), F32), shape((n, d), BF), shape((ne, lo + n), F32)]
    ospecs = [an, an, vm, vm, vm]
    dma = pltpu.SemaphoreType.DMA
    scratch = [pltpu.VMEM((nb, sb, dk, t), BF), pltpu.VMEM((nb, sb, dk, t), BF), pltpu.VMEM((nk, hd, d), BF), pltpu.VMEM((nk, hd, d), BF),
               pltpu.VMEM((ntot if first else n, d), BF), pltpu.VMEM((n, dk), F32), pltpu.VMEM((n, dk), F32),
               pltpu.SMEM(seq_lens.shape, jnp.int32), pltpu.VMEM(expert_ids.shape[::-1], jnp.int32), pltpu.VMEM(ln_moe.shape, BF), pltpu.VMEM(w_router.shape[::-1], BF),
               dma((2, nb)), dma((2, nb)), dma((7,))]
    if first:
        freq = np.power(np.float32(ROPE_BASE), -np.arange(0, hd, 2).astype(np.float32) / np.float32(hd)).astype(np.float32).reshape(-1, 1)
        args += [ln_attn, q_gain, k_gain, jnp.asarray(freq), w_q, w_k, w_v]
        specs += [an]*7
        scratch += [pltpu.VMEM((n, dk), F32), pltpu.VMEM((n, dk), F32), pltpu.VMEM((n//128, dk, 128), F32), pltpu.VMEM((n//128, dk, 128), F32),
                    pltpu.VMEM(w_q.shape, BF), pltpu.VMEM(w_k.shape, BF), pltpu.VMEM(w_v.shape, BF),
                    pltpu.VMEM(seq_lens.shape, jnp.int32), pltpu.VMEM(ln_attn.shape, BF), pltpu.VMEM(q_gain.shape, BF), pltpu.VMEM(k_gain.shape, BF), pltpu.VMEM(freq.shape, F32), dma((8,))]
        if not last:
            m = ntot - n
            outs += [shape((m, dk), F32), shape((m, dk), F32), shape((m//128, dk, 128), F32), shape((m//128, dk, 128), F32)]
            ospecs += [vm]*4
    else:
        args += list(prev)
        specs += [vm]*4 + [an, an, vm]
        alias = {12: 0, 13: 1}
    frac = n / ntot
    return pl.pallas_call(functools.partial(attn_body, cfg + (lo, n, first, last)), out_shape=outs, in_specs=specs, out_specs=ospecs,
        input_output_aliases=alias, scratch_shapes=scratch,
        compiler_params=pltpu.CompilerParams(vmem_limit_bytes=67043328), name="attn",
        cost_estimate=pl.CostEstimate(flops=int(40*10**9*frac), bytes_accessed=int(140*10**6*frac), transcendentals=0),
    )(*args)

def cache_views(c):
    n, t, nk, hd = c.shape
    return c.transpose(0, 2, 3, 1).reshape(n, nk*hd, t), lambda z: z.reshape(n, nk, hd, t).transpose(0, 3, 1, 2)


def moe_body(r_hbm, gt_hbm, y_hbm, wg_own, wu_own, wd_own, wg_par, wu_par, wd_par, out_ref,
             wg, wu, wd, r_ref, gt_ref, xr, gts, y_ref, act, acc, rbuf, wsem, ysem, agsem_s, agsem_r, gsem_s, gsem_r, rssem_s, rssem_r):
    me = lax.axis_index('ep')
    core = me % 2
    xpos = (me // 2) % 2
    ypos = me // 4
    OWN, X, Y, D = 0, 1, 2, 3
    peers = [None, ypos*4 + (1-xpos)*2 + core, (1-ypos)*4 + xpos*2 + core, (1-ypos)*4 + (1-xpos)*2 + core]
    n_loc = wg_own.shape[0]
    n_exp = 2*n_loc
    hr, hc = acc.shape[3], acc.shape[4]
    ff = wg.shape[2]

    mine = [pltpu.make_async_copy(a, b, ysem.at[i]) for i, (a, b) in enumerate(((r_hbm, r_ref), (gt_hbm, gt_ref)))]
    for c in mine:
        c.start()
    barrier = pltpu.get_barrier_semaphore()
    for p in peers[1:]:
        pl.semaphore_signal(barrier, inc=1, device_id={"ep": p}, device_id_type=pl.DeviceIdType.MESH)

    def wcopy(e, own):
        src = (wg_own, wu_own, wd_own) if own else (wg_par, wu_par, wd_par)
        s = lax.rem(e, n_loc)
        return [pltpu.make_async_copy(a.at[s], b.at[e], wsem.at[i, e]) for i, (a, b) in enumerate(zip(src, (wg, wu, wd)))]
    for c in wcopy(jnp.int32(0), True):
        c.start()
    ahead = 2
    for e in range(1, ahead):
        for c in wcopy(jnp.int32(e), True):
            c.start()
    ycopy = pltpu.make_async_copy(y_hbm, y_ref, ysem.at[2])
    for c in mine:
        c.wait()
    pl.semaphore_wait(barrier, 3)

    def remote(src, dst, ss, rs, p):
        return pltpu.make_async_remote_copy(src_ref=src, dst_ref=dst, send_sem=ss, recv_sem=rs,
                                            device_id={"ep": p}, device_id_type=pl.DeviceIdType.MESH)
    ag = {}
    gc = {}
    for b in (D, X, Y):
        rows8 = pl.ds(pl.multiple_of((peers[b] // 2) * n_exp, n_exp), n_exp)
        gc[b] = remote(gt_ref.at[rows8], gts.at[b-1], gsem_s.at[b-1], gsem_r.at[b-1], peers[b])
        gc[b].start()
    for b, h in ((X, 1), (Y, 0), (X, 0), (Y, 1)):
        part = pl.ds(h*hr, hr)
        ag[b, h] = remote(r_ref.at[part], xr.at[b-1, part], agsem_s.at[b-1, h], agsem_r.at[b-1, h], peers[b])
        ag[b, h].start()
    h0, h1 = pl.ds(0, hr), pl.ds(hr, hr)
    relay = [remote(xr.at[Y-1, h0], xr.at[D-1, h0], agsem_s.at[2, 0], agsem_r.at[2, 0], peers[X]),
             remote(xr.at[X-1, h1], xr.at[D-1, h1], agsem_s.at[2, 1], agsem_r.at[2, 1], peers[Y])]

    ycopy.start()

    def gates(b):
        if b == OWN:
            return gt_ref[pl.ds(pl.multiple_of((me // 2) * n_exp, n_exp), n_exp), :].T
        return gts[b-1].T

    def compute(load, g8, blocks, first=False):
        m = len(blocks) * hr
        lane8 = lax.broadcasted_iota(jnp.int32, (m, n_exp), 1)
        for b, h in blocks:
            acc[b, h] = jnp.zeros(acc.shape[2:], F32)
        def step(e, carry):
            if first:
                for c in wcopy(e, True):
                    c.wait()
                @pl.when(e + ahead < n_loc)
                def _():
                    for c in wcopy(e + ahead, True):
                        c.start()
                @pl.when((e + ahead >= n_loc) & (e + ahead < n_exp))
                def _():
                    for c in wcopy(e + ahead, False):
                        c.start()
            gcol = jnp.sum(jnp.where(lane8 == lax.rem(core * n_loc + e, n_exp), g8, 0.0), axis=1, keepdims=True)
            x = load()
            for q in range(2):
                cols = slice(q*ff//2, (q+1)*ff//2)
                g = jnp.dot(x, wg[e, :, cols], preferred_element_type=F32)
                u = jnp.dot(x, wu[e, :, cols], preferred_element_type=F32)
                act[:m, cols] = (jax.nn.silu(g) * u).astype(BF)
            a = act[:m]
            for q in range(4):
                w = hc // 2
                s = (q % 2) * w
                f = jnp.dot(a, wd[e, :, q*w:(q+1)*w], preferred_element_type=F32).astype(BF).astype(F32) * gcol
                for i, (b, h) in enumerate(blocks):
                    acc[b, h, q//2, :, s:s+w] = acc[b, h, q//2, :, s:s+w] + f[i*hr:(i+1)*hr]
            return carry
        lax.fori_loop(0, n_exp, step, 0, unroll=1 if first else 4)

    def rs(i, h, src, p):
        return remote(src, rbuf.at[i, h], rssem_s.at[i, h], rssem_r.at[i, h], p)
    sent = {}
    def send(i, h, src, b):
        sent[i, h] = rs(i, h, src, peers[b])
        sent[i, h].start()

    def rows(h):
        return slice(h*hr, (h+1)*hr)
    def diagonal(h):
        relay[h].wait_recv()
        compute(lambda: xr[D-1, rows(h)], gates(D)[rows(h)], ((D, h),))
        send(0, h, acc.at[D, h, 0], X)
        send(1, h, acc.at[D, h, 1], Y)
    def neighbours(h):
        compute(lambda: jnp.concatenate([xr[X-1, rows(1-h)], xr[Y-1, rows(h)]], axis=0),
                jnp.concatenate([gates(X)[rows(1-h)], gates(Y)[rows(h)]], axis=0), ((X, 1-h), (Y, h)))
        send(2, 1-h, acc.at[X, 1-h, 0], X)
        send(3, h, acc.at[Y, h, 1], Y)
    def own(h, first):
        compute(lambda: r_ref[rows(h)], gates(OWN)[rows(h)], ((OWN, h),), first)
    def pass_on(h):
        sent[1, h].wait_recv()
        acc[X, h, 1] = acc[X, h, 1] + rbuf[1, h]
        send(4, h, acc.at[X, h, 1], X)
        sent[0, h].wait_recv()
        acc[Y, h, 0] = acc[Y, h, 0] + rbuf[0, h]
        send(5, h, acc.at[Y, h, 0], Y)
    own(0, True)
    ag[Y, 0].wait_recv()
    relay[0].start()
    ag[X, 1].wait_recv()
    relay[1].start()
    gc[X].wait_recv(); gc[Y].wait_recv()
    neighbours(0)
    ag[X, 0].wait_recv(); ag[Y, 1].wait_recv()
    neighbours(1)
    gc[D].wait_recv()
    diagonal(0)
    diagonal(1)
    own(1, False)
    pass_on(0)
    pass_on(1)
    ycopy.wait()
    for h in (0, 1):
        sent[2, h].wait_recv()
        sent[3, h].wait_recv()
        acc[OWN, h, 0] = y_ref[rows(h), :hc] + (acc[OWN, h, 0] + rbuf[2, h])
        acc[OWN, h, 1] = y_ref[rows(h), hc:] + (acc[OWN, h, 1] + rbuf[3, h])
        sent[5, h].wait_recv()
        out_ref[rows(h), :hc] = (acc[OWN, h, 0] + rbuf[5, h]).astype(out_ref.dtype)
        sent[4, h].wait_recv()
        out_ref[rows(h), hc:] = (acc[OWN, h, 1] + rbuf[4, h]).astype(out_ref.dtype)
    for c in (*gc.values(), *ag.values(), *relay, *sent.values()):
        c.wait_send()

def moe_call(r, gt, y, w_gate, w_up, w_down, wg_p, wu_p, wd_p):
    n, d = r.shape
    nl, _, ff = w_gate.shape
    vm = pl.BlockSpec(memory_space=pltpu.VMEM)
    an = pl.BlockSpec(memory_space=pl.ANY)
    dma = pltpu.SemaphoreType.DMA
    return pl.pallas_call(moe_body,
        out_shape=jax.ShapeDtypeStruct((n, d), BF),
        in_specs=[an]*9, out_specs=vm,
        scratch_shapes=[pltpu.VMEM((2*nl, d, ff), BF), pltpu.VMEM((2*nl, d, ff), BF), pltpu.VMEM((2*nl, ff, d), BF),
            pltpu.VMEM(r.shape, BF), pltpu.VMEM(gt.shape, F32), pltpu.VMEM((3, n, d), BF), pltpu.VMEM((3, 2*nl, n), F32), pltpu.VMEM((n, d), F32), pltpu.VMEM((n, ff), BF),
            pltpu.VMEM((4, 2, 2, n//2, d//2), F32), pltpu.VMEM((6, 2, n//2, d//2), F32),
            dma((3, 2*nl)), dma((3,)), dma((3, 2)), dma((3, 2)), dma((3,)), dma((3,)), dma((6, 2)), dma((6, 2))],
        compiler_params=pltpu.CompilerParams(vmem_limit_bytes=67043328, collective_id=1, has_side_effects=True), name="moe",
        cost_estimate=pl.CostEstimate(flops=26*10**9, bytes_accessed=30*10**6, transcendentals=0),
    )(r, gt, y, w_gate, w_up, w_down, wg_p, wu_p, wd_p)


def solution(mesh):
    n_group = mesh.shape['ep']
    row_spec = P(('dp', 'ep'), None)
    cache_spec = P(('dp', 'ep'), None, None, None)
    len_spec = P(('dp', 'ep'))
    rep_vec = P(None)
    rep_mat = P(None, None)
    exp_spec = P('ep', None, None)
    swap = [(i, i + 1 - 2 * (i % 2)) for i in range(n_group)]

    def local_step(hidden, k_cache, v_cache, seq_lens, expert_ids, ln_attn, w_q, w_k, w_v, q_gain, k_gain, w_o, ln_moe, w_router, w_gate, w_up, w_down):
        wg_p = lax.ppermute(w_gate, 'ep', swap)
        wu_p = lax.ppermute(w_up, 'ep', swap)
        wd_p = lax.ppermute(w_down, 'ep', swap)
        kc, back = cache_views(k_cache)
        vc, _ = cache_views(v_cache)
        ko, vo, y, r, gt = attn_call(hidden, kc, vc, seq_lens, expert_ids, ln_attn, w_q, w_k, w_v, q_gain, k_gain, w_o, ln_moe, w_router, 0, hidden.shape[0])
        out = moe_call(r, gt, y, w_gate, w_up, w_down, wg_p, wu_p, wd_p)
        return out, back(ko), back(vo)

    return jax.shard_map(local_step, mesh=mesh, in_specs=(row_spec, cache_spec, cache_spec, len_spec, row_spec, rep_vec, rep_mat, rep_mat, rep_mat, rep_vec, rep_vec, rep_mat, rep_vec, rep_mat, exp_spec, exp_spec, exp_spec), out_specs=(row_spec, cache_spec, cache_spec), check_vma=False)
```
